8 devices in a mesh: dp: 2 (over z, y), ep: 4 (over x, core).
Axes of the slice: x: 2, y: 2, z: 1, core: 2. Of those that a mesh axis runs over, the one named last changes fastest.
Arguments:
- x_tokens: bfloat16 [16, 1024, 1024], P(('dp', 'ep'))
- dy_tokens: bfloat16 [16, 1024, 1024], P(('dp', 'ep'))
- route_idx: int32 [16, 1024, 8], P(('dp', 'ep'))
- norm1_gain: bfloat16 [1024], replicated
- norm2_gain: bfloat16 [1024], replicated
- w_qkv: bfloat16 [1024, 3072], replicated
- w_attn_out: bfloat16 [1024, 1024], replicated
- w_router: bfloat16 [1024, 64], replicated
- w_gate: bfloat16 [64, 1024, 1024], P('ep')
- w_up: bfloat16 [64, 1024, 1024], P('ep')
- w_down: bfloat16 [64, 1024, 1024], P('ep')
Outputs:
- output 1: bfloat16 [16, 1024, 1024], P(('dp', 'ep'))
- output 2: float32 [1024], replicated
- output 3: float32 [1024], replicated
- output 4: float32 [1024, 3072], replicated
- output 5: float32 [1024, 1024], replicated
- output 6: float32 [1024, 64], replicated
- output 7: float32 [64, 1024, 1024], P('ep')
- output 8: float32 [64, 1024, 1024], P('ep')
- output 9: float32 [64, 1024, 1024], P('ep')
All inputs are finite; a program needn't handle non-finite values.
Results may differ from the reference program's by a relative error of at most 0.0178083.
Values are sent between devices in bfloat16 or wider.
A program may use at most 1.5 GiB of HBM per device.

```python
import jax
import jax.numpy as jnp
from jax import lax

D = 1024
HEAD_DIM = 128
FF = 1024
EXPERTS = 64
TOP = 8
SEQ = 1024
SEQS = 2
DEVICES = 8

TOKENS = SEQS * SEQ
BATCH = DEVICES * SEQS
CAP = 8 * ((5 * TOKENS * TOP + 32 * EXPERTS - 1) // (32 * EXPERTS))
HOT_ROWS = CAP + CAP // 4
EPS = 1e-6
ROPE_BASE = 10000.0


def draw_routes(route_key):
    score_key, hot_key = jax.random.split(route_key)
    base_scores = jax.random.randint(score_key, (BATCH, SEQ, EXPERTS), 0, 2 ** 20, jnp.int32)
    hot_expert = jax.random.randint(hot_key, (DEVICES,), 0, EXPERTS, jnp.int32)
    expert_ids = jnp.arange(EXPERTS, dtype=jnp.int32)
    seq_ids = jnp.arange(BATCH, dtype=jnp.int32)
    local_pos = (seq_ids % SEQS)[:, None] * SEQ + jnp.arange(SEQ, dtype=jnp.int32)[None, :]
    hot_of_seq = hot_expert[seq_ids // SEQS]
    forced = (local_pos < HOT_ROWS)[:, :, None] & (expert_ids[None, None, :] == hot_of_seq[:, None, None])
    scores = base_scores * EXPERTS + expert_ids[None, None, :] + jnp.where(forced, 2 ** 29, 0)
    return lax.top_k(scores, TOP)[1].astype(jnp.int32)


def scaled_normal(draw_key, shape_dims, factor):
    return (jax.random.normal(draw_key, shape_dims, jnp.float32) * factor).astype(jnp.bfloat16)


def setup_inputs(seed: int = 0) -> dict:
    key_list = jax.random.split(jax.random.key(seed), 11)
    return {
        'x_tokens': scaled_normal(key_list[0], (BATCH, SEQ, D), 1.0),
        'dy_tokens': scaled_normal(key_list[1], (BATCH, SEQ, D), 1.0),
        'route_idx': draw_routes(key_list[2]),
        'norm1_gain': (1.0 + 0.3 * jax.random.normal(key_list[3], (D,), jnp.float32)).astype(jnp.bfloat16),
        'norm2_gain': (1.0 + 0.3 * jax.random.normal(key_list[4], (D,), jnp.float32)).astype(jnp.bfloat16),
        'w_qkv': scaled_normal(key_list[5], (D, 3 * D), D ** -0.5),
        'w_attn_out': scaled_normal(key_list[6], (D, D), D ** -0.5),
        'w_router': scaled_normal(key_list[7], (D, EXPERTS), D ** -0.5),
        'w_gate': scaled_normal(key_list[8], (EXPERTS, D, FF), D ** -0.5),
        'w_up': scaled_normal(key_list[9], (EXPERTS, D, FF), D ** -0.5),
        'w_down': scaled_normal(key_list[10], (EXPERTS, FF, D), FF ** -0.5),
    }


def mat_f32(left, right):
    return jnp.dot(left.astype(jnp.float32), right.astype(jnp.float32), preferred_element_type=jnp.float32)


def rms_norm(x_rows, gain_vec):
    x_f32 = x_rows.astype(jnp.float32)
    inv_rms = lax.rsqrt(jnp.mean(x_f32 * x_f32, axis=-1, keepdims=True) + EPS)
    return (x_f32 * inv_rms * gain_vec.astype(jnp.float32)).astype(jnp.bfloat16)


def rope_rotate(head_vals):
    seq_len = head_vals.shape[1]
    half_dim = head_vals.shape[-1] // 2
    inv_freq = ROPE_BASE ** (-jnp.arange(half_dim, dtype=jnp.float32) / half_dim)
    angles = jnp.arange(seq_len, dtype=jnp.float32)[:, None] * inv_freq[None, :]
    cos_b = jnp.cos(angles)[None, :, None, :]
    sin_b = jnp.sin(angles)[None, :, None, :]
    lower_half = head_vals[..., :half_dim]
    upper_half = head_vals[..., half_dim:]
    return jnp.concatenate([lower_half * cos_b - upper_half * sin_b, upper_half * cos_b + lower_half * sin_b], axis=-1)


def gate_probs(logits, idx_rows):
    probs_all = jax.nn.softmax(logits, axis=-1)
    picked = jnp.take_along_axis(probs_all, idx_rows, axis=1)
    return picked / jnp.sum(picked, axis=1, keepdims=True)


def route_slots(idx_rows, num_experts, capacity):
    num_tokens, top_k = idx_rows.shape
    hit_count = jnp.sum((idx_rows[:, :, None] == jnp.arange(num_experts)[None, None, :]).astype(jnp.int32), axis=1)
    earlier = jnp.cumsum(hit_count, axis=0) - hit_count
    position = jnp.take_along_axis(earlier, idx_rows, axis=1)
    slot_ids = jnp.where(position < capacity, idx_rows * capacity + position, num_experts * capacity)
    source_ids = jnp.full((num_experts * capacity,), num_tokens * top_k, jnp.int32).at[slot_ids.reshape(-1)].set(jnp.arange(num_tokens * top_k, dtype=jnp.int32), mode='drop')
    return slot_ids, source_ids


def take_rows(table, row_ids):
    return jnp.take(table, row_ids, axis=0, mode='fill', fill_value=0)


def device_layer(weight_set, x_rows, idx_rows):
    norm1_gain, norm2_gain, w_qkv, w_attn_out, w_router, w_gate, w_up, w_down = weight_set
    normed1 = rms_norm(x_rows, norm1_gain)
    qkv_heads = mat_f32(normed1, w_qkv).reshape(SEQS, SEQ, 3, D // HEAD_DIM, HEAD_DIM)
    query_rot = rope_rotate(qkv_heads[:, :, 0]).astype(jnp.bfloat16).astype(jnp.float32)
    key_rot = rope_rotate(qkv_heads[:, :, 1]).astype(jnp.bfloat16).astype(jnp.float32)
    value_h = qkv_heads[:, :, 2].astype(jnp.bfloat16).astype(jnp.float32)
    scores = jnp.einsum('bqhd,bkhd->bhqk', query_rot, key_rot) * HEAD_DIM ** -0.5
    causal = jnp.arange(SEQ)[:, None] >= jnp.arange(SEQ)[None, :]
    attn_probs = jax.nn.softmax(jnp.where(causal, scores, -1e30), axis=-1).astype(jnp.bfloat16).astype(jnp.float32)
    context = jnp.einsum('bhqk,bkhd->bqhd', attn_probs, value_h).astype(jnp.bfloat16).reshape(TOKENS, D)
    h_rows = (x_rows.astype(jnp.float32) + mat_f32(context, w_attn_out)).astype(jnp.bfloat16)
    normed2 = rms_norm(h_rows, norm2_gain)
    gate_vals = gate_probs(mat_f32(normed2, w_router), idx_rows)
    slot_ids, source_ids = route_slots(idx_rows, EXPERTS, CAP)
    slot_rows = take_rows(normed2, source_ids // TOP).reshape(EXPERTS, CAP, D).astype(jnp.float32)
    act_gate = jnp.einsum('ecd,edf->ecf', slot_rows, w_gate)
    act_up = jnp.einsum('ecd,edf->ecf', slot_rows, w_up)
    hidden = (jax.nn.silu(act_gate) * act_up).astype(jnp.bfloat16).astype(jnp.float32)
    expert_out = jnp.einsum('ecf,efd->ecd', hidden, w_down).astype(jnp.bfloat16).reshape(EXPERTS * CAP, D)
    choice_rows = take_rows(expert_out, slot_ids.reshape(-1)).reshape(TOKENS, TOP, D)
    moe_out = jnp.sum(gate_vals[:, :, None] * choice_rows.astype(jnp.float32), axis=1)
    return (h_rows.astype(jnp.float32) + moe_out).astype(jnp.bfloat16)


def reference(x_tokens, dy_tokens, route_idx, norm1_gain, norm2_gain, w_qkv, w_attn_out, w_router, w_gate, w_up, w_down):
    weight_set = tuple(weight_arr.astype(jnp.float32) for weight_arr in (norm1_gain, norm2_gain, w_qkv, w_attn_out, w_router, w_gate, w_up, w_down))
    x_dev = x_tokens.reshape(DEVICES, TOKENS, D)
    dy_dev = dy_tokens.reshape(DEVICES, TOKENS, D)
    idx_dev = route_idx.reshape(DEVICES, TOKENS, TOP)

    def device_step(totals, per_device):
        x_rows, dy_rows, idx_rows = per_device
        pullback = jax.vjp(lambda weights_in, x_in: device_layer(weights_in, x_in, idx_rows), weight_set, x_rows)[1]
        d_weights, d_x = pullback(dy_rows)
        return jax.tree.map(lambda a, b: a + b, totals, d_weights), d_x

    zero_set = tuple(jnp.zeros_like(weight_arr) for weight_arr in weight_set)
    totals, d_x_dev = lax.scan(device_step, zero_set, (x_dev, dy_dev, idx_dev))
    return (d_x_dev.reshape(x_tokens.shape), totals[0], totals[1], totals[2], totals[3], totals[4], totals[5], totals[6], totals[7])
```

```python
import functools

import jax
import jax.numpy as jnp
from jax import lax
from jax.experimental import pallas as pl
from jax.experimental.pallas import tpu as pltpu
from jax.sharding import PartitionSpec as P

EPS = 1e-6
HEAD_DIM = 128
ROPE_BASE = 10000.0
TOK_BLOCK = 256
WIN = 64
ALIGN = 16
VMEM_MAX = 64 * 1024 * 1024 - 65536


def capacity_rows(num_tokens, top_k, num_experts):
    return 8 * ((5 * num_tokens * top_k + 32 * num_experts - 1) // (32 * num_experts))


def rms_norm(x_rows, gain_vec):
    x_f32 = x_rows.astype(jnp.float32)
    inv_rms = lax.rsqrt(jnp.mean(x_f32 * x_f32, axis=-1, keepdims=True) + EPS)
    return (x_f32 * inv_rms * gain_vec.astype(jnp.float32)).astype(jnp.bfloat16)


def rms_norm_bwd(x_rows, gain_vec, d_out):
    x_f32 = x_rows.astype(jnp.float32)
    inv_rms = lax.rsqrt(jnp.mean(x_f32 * x_f32, axis=-1, keepdims=True) + EPS)
    d_gain = jnp.sum(d_out * x_f32 * inv_rms, axis=0)
    d_scaled = d_out * gain_vec.astype(jnp.float32)
    d_x = inv_rms * d_scaled - x_f32 * inv_rms ** 3 * jnp.mean(d_scaled * x_f32, axis=-1, keepdims=True)
    return d_x, d_gain


def rope_rotate(head_vals):
    seq_len = head_vals.shape[1]
    half_dim = head_vals.shape[-1] // 2
    inv_freq = ROPE_BASE ** (-jnp.arange(half_dim, dtype=jnp.float32) / half_dim)
    angles = jnp.arange(seq_len, dtype=jnp.float32)[:, None] * inv_freq[None, :]
    cos_b = jnp.cos(angles)[None, :, None, :]
    sin_b = jnp.sin(angles)[None, :, None, :]
    lower_half = head_vals[..., :half_dim]
    upper_half = head_vals[..., half_dim:]
    return jnp.concatenate([lower_half * cos_b - upper_half * sin_b, upper_half * cos_b + lower_half * sin_b], axis=-1)


def attention_core(qkv_rows, num_seqs):
    num_tokens = qkv_rows.shape[0]
    seq_len = num_tokens // num_seqs
    model_width = qkv_rows.shape[1] // 3
    qkv_heads = qkv_rows.reshape(num_seqs, seq_len, 3, model_width // HEAD_DIM, HEAD_DIM)
    query_rot = rope_rotate(qkv_heads[:, :, 0]).astype(jnp.bfloat16)
    key_rot = rope_rotate(qkv_heads[:, :, 1]).astype(jnp.bfloat16)
    value_h = qkv_heads[:, :, 2].astype(jnp.bfloat16)
    scores = jnp.einsum('bqhd,bkhd->bhqk', query_rot, key_rot, preferred_element_type=jnp.float32) * HEAD_DIM ** -0.5
    causal = jnp.arange(seq_len)[:, None] >= jnp.arange(seq_len)[None, :]
    attn_probs = jax.nn.softmax(jnp.where(causal, scores, -1e30), axis=-1).astype(jnp.bfloat16)
    context = jnp.einsum('bhqk,bkhd->bqhd', attn_probs, value_h, preferred_element_type=jnp.float32)
    return context.astype(jnp.bfloat16).reshape(num_tokens, model_width)


def choice_mask(idx_rows, num_experts):
    return (idx_rows[:, :, None] == jnp.arange(num_experts, dtype=jnp.int32)[None, None, :])


def gate_forward(logits, idx_rows, num_experts):
    probs_all = jax.nn.softmax(logits, axis=-1)
    hits = jnp.sum(choice_mask(idx_rows, num_experts).astype(jnp.float32), axis=1)
    picked_sum = jnp.sum(probs_all * hits, axis=1, keepdims=True)
    return probs_all, hits, picked_sum


def gate_backward(probs_all, hits, picked_sum, d_gate_dense):
    gates = probs_all * hits / picked_sum
    d_probs = hits * (d_gate_dense - jnp.sum(d_gate_dense * gates, axis=1, keepdims=True)) / picked_sum
    return probs_all * (d_probs - jnp.sum(d_probs * probs_all, axis=1, keepdims=True))


def slot_positions(idx_t, first_expert, local_experts, capacity):
    num_dev, _, num_tokens = idx_t.shape
    experts = first_expert + jnp.arange(local_experts, dtype=jnp.int32)
    hits = jnp.sum((idx_t[:, None, :, :] == experts[None, :, None, None]).astype(jnp.float32), axis=2)
    blocks = num_tokens // TOK_BLOCK
    hit_blk = hits.reshape(num_dev, local_experts, blocks, TOK_BLOCK)
    upto = (jnp.arange(TOK_BLOCK)[:, None] <= jnp.arange(TOK_BLOCK)[None, :]).astype(jnp.bfloat16)
    within = jnp.einsum('debt,tu->debu', hit_blk.astype(jnp.bfloat16), upto, preferred_element_type=jnp.float32)
    totals = jnp.sum(hit_blk, axis=-1)
    strict = (jnp.arange(blocks)[:, None] < jnp.arange(blocks)[None, :])
    before = jnp.sum(jnp.where(strict[None, None], totals[:, :, :, None], 0.0), axis=2)
    position = (within + before[..., None] - 1.0).astype(jnp.int32)
    slot_of = jnp.where((hit_blk > 0) & (position < capacity), position, -1).reshape(num_dev, local_experts, num_tokens)
    begin = jnp.minimum(before.astype(jnp.int32), capacity)
    end = jnp.minimum((before + totals).astype(jnp.int32), capacity)
    win_start = jnp.minimum(begin // ALIGN * ALIGN, capacity - WIN)
    win_count = jnp.maximum((end - win_start + WIN - 1) // WIN, 1)
    return slot_of, win_start.reshape(-1), win_count.reshape(-1)


def gather_kernel(base_ref, start_ref, count_ref, x_ref, dy_ref, slot_ref, gate_ref, s_ref, dyr_ref, g_ref, *, experts, blocks, capacity, group):
    dev, blk = pl.program_id(0), pl.program_id(1)

    @pl.when(blk == 0)
    def _():
        s_ref[...] = jnp.zeros_like(s_ref)
        dyr_ref[...] = jnp.zeros_like(dyr_ref)
        g_ref[...] = jnp.zeros_like(g_ref)

    row_iota = lax.broadcasted_iota(jnp.int32, (WIN, TOK_BLOCK), 0)

    def window(e, first, floor):
        slot_row = slot_ref[0, e:e + 1, :]
        hit = (slot_row == row_iota + first) & (slot_row >= floor)
        gate_col = jnp.sum(jnp.where(hit, gate_ref[0, e:e + 1, :], 0.0), axis=1, keepdims=True)
        return jnp.where(hit, 1.0, 0.0).astype(jnp.bfloat16), gate_col

    def deposit(e, first, s_rows, dy_rows, gate_col):
        rows = pl.ds(pl.multiple_of(first, ALIGN), WIN)
        s_ref[e, 0, rows, :] += s_rows.astype(jnp.bfloat16)
        dyr_ref[e, 0, rows, :] += dy_rows.astype(jnp.bfloat16)
        g_ref[e, 0, rows, :] += gate_col

    for e0 in range(0, experts, group):
        firsts = [start_ref[(dev * experts + e0 + i) * blocks + blk] for i in range(group)]
        parts = [window(e0 + i, firsts[i], 0) for i in range(group)]
        pick = jnp.concatenate([p[0] for p in parts], axis=0)
        s_all = jnp.dot(pick, x_ref[...], preferred_element_type=jnp.float32)
        dy_all = jnp.dot(pick, dy_ref[...], preferred_element_type=jnp.float32)
        for i in range(group):
            rows = slice(i * WIN, (i + 1) * WIN)
            deposit(e0 + i, firsts[i], s_all[rows], dy_all[rows], parts[i][1])

    for e in range(experts):
        at = (dev * experts + e) * blocks + blk
        count = count_ref[at]

        @pl.when(count > 1)
        def _():
            def extra(w, carry):
                floor = start_ref[at] + w * WIN
                first = jnp.minimum(floor, capacity - WIN)
                pick, gate_col = window(e, first, floor)
                s_rows = jnp.dot(pick, x_ref[...], preferred_element_type=jnp.float32)
                dy_rows = jnp.dot(pick, dy_ref[...], preferred_element_type=jnp.float32)
                deposit(e, first, s_rows, dy_rows, gate_col)
                return carry
            lax.fori_loop(1, count, extra, 0)


def gather_slots(base_dev, win_start, win_count, x_all, dy_all, slot_of, gate_of, capacity):
    num_dev, experts, num_tokens = slot_of.shape
    width = x_all.shape[1]
    blocks = num_tokens // TOK_BLOCK

    def table_map(d, b, base_ref, start_ref, count_ref):
        return (lax.rem(d + base_ref[0], num_dev) * blocks + b, 0)

    def route_map(d, b, *_):
        return (d, 0, b)

    def out_map(d, b, *_):
        return (0, d, 0, 0)

    return pl.pallas_call(
        functools.partial(gather_kernel, experts=experts, blocks=blocks, capacity=capacity, group=4),
        out_shape=[jax.ShapeDtypeStruct((experts, num_dev, capacity, width), jnp.bfloat16),
                   jax.ShapeDtypeStruct((experts, num_dev, capacity, width), jnp.bfloat16),
                   jax.ShapeDtypeStruct((experts, num_dev, capacity, 1), jnp.float32)],
        grid_spec=pltpu.PrefetchScalarGridSpec(
            num_scalar_prefetch=3, grid=(num_dev, blocks),
            in_specs=[pl.BlockSpec((TOK_BLOCK, width), table_map), pl.BlockSpec((TOK_BLOCK, width), table_map),
                      pl.BlockSpec((1, experts, TOK_BLOCK), route_map), pl.BlockSpec((1, experts, TOK_BLOCK), route_map)],
            out_specs=[pl.BlockSpec((experts, 1, capacity, width), out_map), pl.BlockSpec((experts, 1, capacity, width), out_map),
                       pl.BlockSpec((experts, 1, capacity, 1), out_map)]),
        compiler_params=pltpu.CompilerParams(vmem_limit_bytes=VMEM_MAX, dimension_semantics=('arbitrary', 'arbitrary')),
        cost_estimate=pl.CostEstimate(flops=4 * num_dev * blocks * experts * WIN * TOK_BLOCK * width,
                                      bytes_accessed=4 * num_dev * (num_tokens + experts * capacity) * width, transcendentals=0),
        name='gather_slots',
    )(base_dev, win_start, win_count, x_all, dy_all, slot_of, gate_of)


def combine_kernel(start_ref, count_ref, ds_ref, dg_ref, slot_ref, out_ref, dgt_ref, *, experts, blocks, capacity, group):
    dev, blk = pl.program_id(0), pl.program_id(1)
    row_iota = lax.broadcasted_iota(jnp.int32, (WIN, TOK_BLOCK), 0)

    def window(e, first, floor):
        slot_row = slot_ref[0, e:e + 1, :]
        hit = (slot_row == row_iota + first) & (slot_row >= floor)
        rows = pl.ds(pl.multiple_of(first, ALIGN), WIN)
        gate_row = jnp.sum(jnp.where(hit, dg_ref[e, 0, rows, :], 0.0), axis=0, keepdims=True)
        return jnp.where(hit, 1.0, 0.0).astype(jnp.bfloat16), ds_ref[e, 0, rows, :], gate_row

    def spread(pick, rows):
        return lax.dot_general(pick, rows, (((0,), (0,)), ((), ())), preferred_element_type=jnp.float32)

    for e0 in range(0, experts, group):
        parts = [window(e0 + i, start_ref[(dev * experts + e0 + i) * blocks + blk], 0) for i in range(group)]
        total = spread(jnp.concatenate([p[0] for p in parts], axis=0), jnp.concatenate([p[1] for p in parts], axis=0))
        out_ref[...] = total if e0 == 0 else out_ref[...] + total
        for i in range(group):
            dgt_ref[0, e0 + i:e0 + i + 1, :] = parts[i][2]

    for e in range(experts):
        at = (dev * experts + e) * blocks + blk
        count = count_ref[at]

        @pl.when(count > 1)
        def _():
            def extra(w, carry):
                floor = start_ref[at] + w * WIN
                pick, rows, gate_row = window(e, jnp.minimum(floor, capacity - WIN), floor)
                out_ref[...] += spread(pick, rows)
                dgt_ref[0, e:e + 1, :] += gate_row
                return carry
            lax.fori_loop(1, count, extra, 0)


def combine_slots(win_start, win_count, d_slots, d_gate_slots, slot_of, num_dev):
    experts, _, capacity, width = d_slots.shape
    num_tokens = slot_of.shape[-1]
    blocks = num_tokens // TOK_BLOCK
    return pl.pallas_call(
        functools.partial(combine_kernel, experts=experts, blocks=blocks, capacity=capacity, group=4),
        out_shape=[jax.ShapeDtypeStruct((num_dev * num_tokens, width), jnp.float32),
                   jax.ShapeDtypeStruct((num_dev, experts, num_tokens), jnp.float32)],
        grid_spec=pltpu.PrefetchScalarGridSpec(
            num_scalar_prefetch=2, grid=(num_dev, blocks),
            in_specs=[pl.BlockSpec((experts, 1, capacity, width), lambda d, b, *_: (0, d, 0, 0)),
                      pl.BlockSpec((experts, 1, capacity, 1), lambda d, b, *_: (0, d, 0, 0)),
                      pl.BlockSpec((1, experts, TOK_BLOCK), lambda d, b, *_: (d, 0, b))],
            out_specs=[pl.BlockSpec((TOK_BLOCK, width), lambda d, b, *_: (d * blocks + b, 0)),
                       pl.BlockSpec((1, experts, TOK_BLOCK), lambda d, b, *_: (d, 0, b))]),
        compiler_params=pltpu.CompilerParams(vmem_limit_bytes=VMEM_MAX, dimension_semantics=('arbitrary', 'arbitrary')),
        cost_estimate=pl.CostEstimate(flops=2 * num_dev * blocks * experts * WIN * TOK_BLOCK * width,
                                      bytes_accessed=2 * num_dev * (2 * num_tokens + experts * capacity) * width, transcendentals=0),
        name='combine_slots',
    )(win_start, win_count, d_slots, d_gate_slots, slot_of)


def dense_backward(saved_state, x_rows, dy_rows, d_logits, d_normed2_moe, norm1_gain, norm2_gain, w_qkv, w_attn_out, w_router):
    normed1, attn_pullback, context, h_rows, normed2 = saved_state
    d_w_router = jnp.einsum('td,te->de', normed2, d_logits, preferred_element_type=jnp.float32)
    d_normed2 = d_normed2_moe + jnp.einsum('te,de->td', d_logits, w_router, preferred_element_type=jnp.float32)
    d_h_part, d_norm2_gain = rms_norm_bwd(h_rows, norm2_gain, d_normed2)
    d_h = (dy_rows.astype(jnp.float32) + d_h_part).astype(jnp.bfloat16)
    d_w_attn_out = jnp.einsum('td,te->de', context, d_h, preferred_element_type=jnp.float32)
    d_context = jnp.einsum('te,de->td', d_h, w_attn_out, preferred_element_type=jnp.float32).astype(jnp.bfloat16)
    d_qkv = attn_pullback(d_context)[0].astype(jnp.bfloat16)
    d_w_qkv = jnp.einsum('td,te->de', normed1, d_qkv, preferred_element_type=jnp.float32)
    d_normed1 = jnp.einsum('te,de->td', d_qkv, w_qkv, preferred_element_type=jnp.float32)
    d_x_part, d_norm1_gain = rms_norm_bwd(x_rows, norm1_gain, d_normed1)
    d_x = (d_h.astype(jnp.float32) + d_x_part).astype(jnp.bfloat16)
    return d_x, (d_norm1_gain, d_norm2_gain, d_w_qkv, d_w_attn_out, d_w_router)


def solution(mesh):
    ep_size, dp_size = mesh.shape['ep'], mesh.shape['dp']
    num_dev = ep_size * dp_size
    tok_spec = P(('dp', 'ep'), None, None)
    rep_spec = P()
    exp_spec = P('ep', None, None)

    def local_step(x_tokens, dy_tokens, route_idx, norm1_gain, norm2_gain, w_qkv, w_attn_out, w_router, w_gate, w_up, w_down):
        num_seqs, seq_len, model_width = x_tokens.shape
        num_tokens = num_seqs * seq_len
        top_k = route_idx.shape[-1]
        local_experts = w_gate.shape[0]
        num_experts = local_experts * ep_size
        capacity = capacity_rows(num_tokens, top_k, num_experts)
        x_rows = x_tokens.reshape(num_tokens, model_width)
        dy_rows = dy_tokens.reshape(num_tokens, model_width)
        idx_rows = route_idx.reshape(num_tokens, top_k)
        base = lax.axis_index('dp') * ep_size

        dy_all = lax.all_gather(dy_rows, ('dp', 'ep'), axis=0, tiled=True)
        idx_all = lax.all_gather(idx_rows.T, ('dp', 'ep'), axis=0)
        idx_all = jnp.roll(idx_all, -base, axis=0)
        slot_of, win_start, win_count = slot_positions(idx_all, lax.axis_index('ep') * local_experts, local_experts, capacity)

        normed1 = rms_norm(x_rows, norm1_gain)
        qkv_rows = jnp.dot(normed1, w_qkv, preferred_element_type=jnp.float32)
        context, attn_pullback = jax.vjp(lambda qkv_in: attention_core(qkv_in, num_seqs), qkv_rows)
        h_rows = (x_rows.astype(jnp.float32) + jnp.dot(context, w_attn_out, preferred_element_type=jnp.float32)).astype(jnp.bfloat16)
        normed2 = rms_norm(h_rows, norm2_gain)
        x_all = lax.all_gather(normed2, ('dp', 'ep'), axis=0, tiled=True)
        logits = jnp.dot(normed2, w_router, preferred_element_type=jnp.float32)
        probs_all, hits, picked_sum = gate_forward(logits, idx_rows, num_experts)
        gate_t = jnp.transpose(probs_all * hits / picked_sum)
        gate_all = lax.all_gather(gate_t.reshape(ep_size, local_experts, num_tokens), ('dp', 'ep'), axis=0)
        gate_of = jnp.roll(lax.dynamic_index_in_dim(gate_all, lax.axis_index('ep'), axis=1, keepdims=False), -base, axis=0)

        slots, dy_slots, gate_slots = gather_slots(base[None], win_start, win_count, x_all, dy_all, slot_of, gate_of, capacity)
        own = ep_size * capacity
        rows_of = lambda a: a.reshape(local_experts, num_dev * capacity, a.shape[-1])
        s_all, dy_s, g_s = rows_of(slots), rows_of(dy_slots), rows_of(gate_slots)
        mm = functools.partial(jnp.einsum, preferred_element_type=jnp.float32)
        act_gate = mm('ecd,edf->ecf', s_all, w_gate)
        act_up = mm('ecd,edf->ecf', s_all, w_up)
        hidden = (jax.nn.silu(act_gate) * act_up).astype(jnp.bfloat16)
        expert_out = mm('ecf,efd->ecd', hidden[:, :own], w_down).astype(jnp.bfloat16)
        d_gate_slots = jnp.sum(dy_s[:, :own].astype(jnp.float32) * expert_out.astype(jnp.float32), axis=-1, keepdims=True)
        d_out = (dy_s.astype(jnp.float32) * g_s).astype(jnp.bfloat16)
        d_hidden = mm('ecd,efd->ecf', d_out, w_down)
        sigmoid_g = jax.nn.sigmoid(act_gate)
        d_act_up = (d_hidden * act_gate * sigmoid_g).astype(jnp.bfloat16)
        d_act_gate = (d_hidden * act_up * sigmoid_g * (1.0 + act_gate * (1.0 - sigmoid_g))).astype(jnp.bfloat16)
        d_slots = (mm('ecf,edf->ecd', d_act_gate[:, :own], w_gate) + mm('ecf,edf->ecd', d_act_up[:, :own], w_up)).astype(jnp.bfloat16)
        d_tok, d_gate_t = combine_slots(win_start, win_count, d_slots.reshape(local_experts, ep_size, capacity, model_width),
                                        d_gate_slots.reshape(local_experts, ep_size, capacity, 1), slot_of, ep_size)
        d_normed2_moe = lax.psum_scatter(d_tok, 'ep', scatter_dimension=0, tiled=True)
        d_gate_dense = jnp.transpose(lax.all_to_all(d_gate_t, 'ep', 0, 0, tiled=True).reshape(num_experts, num_tokens))
        d_w_down = mm('ecf,ecd->efd', hidden, d_out)
        d_w_gate = mm('ecd,ecf->edf', s_all, d_act_gate)
        d_w_up = mm('ecd,ecf->edf', s_all, d_act_up)

        d_logits = gate_backward(probs_all, hits, picked_sum, d_gate_dense).astype(jnp.bfloat16)
        saved_state = (normed1, attn_pullback, context, h_rows, normed2)
        d_x, dense_grads = dense_backward(saved_state, x_rows, dy_rows, d_logits, d_normed2_moe, norm1_gain, norm2_gain, w_qkv, w_attn_out, w_router)
        dense_grads = lax.psum(dense_grads, ('dp', 'ep'))
        return (d_x.reshape(x_tokens.shape),) + tuple(dense_grads) + (d_w_gate, d_w_up, d_w_down)

    return jax.shard_map(local_step, mesh=mesh,
                         in_specs=(tok_spec, tok_spec, tok_spec, rep_spec, rep_spec, rep_spec, rep_spec, rep_spec, exp_spec, exp_spec, exp_spec),
                         out_specs=(tok_spec, rep_spec, rep_spec, rep_spec, rep_spec, rep_spec, exp_spec, exp_spec, exp_spec),
                         check_vma=False)
```

```python
import functools

import jax
import jax.numpy as jnp
from jax import lax
from jax.experimental import pallas as pl
from jax.experimental.pallas import tpu as pltpu
from jax.sharding import PartitionSpec as P

EPS = 1e-6
HEAD_DIM = 128
ROPE_BASE = 10000.0
TOK_BLOCK = 256
WIN = 64
ALIGN = 16
VMEM_MAX = 64 * 1024 * 1024 - 65536


def capacity_rows(num_tokens, top_k, num_experts):
    return 8 * ((5 * num_tokens * top_k + 32 * num_experts - 1) // (32 * num_experts))


def rms_norm(x_rows, gain_vec):
    x_f32 = x_rows.astype(jnp.float32)
    inv_rms = lax.rsqrt(jnp.mean(x_f32 * x_f32, axis=-1, keepdims=True) + EPS)
    return (x_f32 * inv_rms * gain_vec.astype(jnp.float32)).astype(jnp.bfloat16)


def rms_norm_bwd(x_rows, gain_vec, d_out):
    x_f32 = x_rows.astype(jnp.float32)
    inv_rms = lax.rsqrt(jnp.mean(x_f32 * x_f32, axis=-1, keepdims=True) + EPS)
    d_gain = jnp.sum(d_out * x_f32 * inv_rms, axis=0)
    d_scaled = d_out * gain_vec.astype(jnp.float32)
    d_x = inv_rms * d_scaled - x_f32 * inv_rms ** 3 * jnp.mean(d_scaled * x_f32, axis=-1, keepdims=True)
    return d_x, d_gain


def rope_rotate(head_vals):
    seq_len = head_vals.shape[1]
    half_dim = head_vals.shape[-1] // 2
    inv_freq = ROPE_BASE ** (-jnp.arange(half_dim, dtype=jnp.float32) / half_dim)
    angles = jnp.arange(seq_len, dtype=jnp.float32)[:, None] * inv_freq[None, :]
    cos_b = jnp.cos(angles)[None, :, None, :]
    sin_b = jnp.sin(angles)[None, :, None, :]
    lower_half = head_vals[..., :half_dim]
    upper_half = head_vals[..., half_dim:]
    return jnp.concatenate([lower_half * cos_b - upper_half * sin_b, upper_half * cos_b + lower_half * sin_b], axis=-1)


def attention_core(qkv_rows, num_seqs):
    num_tokens = qkv_rows.shape[0]
    seq_len = num_tokens // num_seqs
    model_width = qkv_rows.shape[1] // 3
    qkv_heads = qkv_rows.reshape(num_seqs, seq_len, 3, model_width // HEAD_DIM, HEAD_DIM)
    query_rot = rope_rotate(qkv_heads[:, :, 0]).astype(jnp.bfloat16)
    key_rot = rope_rotate(qkv_heads[:, :, 1]).astype(jnp.bfloat16)
    value_h = qkv_heads[:, :, 2].astype(jnp.bfloat16)
    scores = jnp.einsum('bqhd,bkhd->bhqk', query_rot, key_rot, preferred_element_type=jnp.float32) * HEAD_DIM ** -0.5
    causal = jnp.arange(seq_len)[:, None] >= jnp.arange(seq_len)[None, :]
    attn_probs = jax.nn.softmax(jnp.where(causal, scores, -1e30), axis=-1).astype(jnp.bfloat16)
    context = jnp.einsum('bhqk,bkhd->bqhd', attn_probs, value_h, preferred_element_type=jnp.float32)
    return context.astype(jnp.bfloat16).reshape(num_tokens, model_width)


def choice_mask(idx_rows, num_experts):
    return (idx_rows[:, :, None] == jnp.arange(num_experts, dtype=jnp.int32)[None, None, :])


def gate_forward(logits, idx_rows, num_experts):
    probs_all = jax.nn.softmax(logits, axis=-1)
    hits = jnp.sum(choice_mask(idx_rows, num_experts).astype(jnp.float32), axis=1)
    picked_sum = jnp.sum(probs_all * hits, axis=1, keepdims=True)
    return probs_all, hits, picked_sum


def gate_backward(probs_all, hits, picked_sum, d_gate_dense):
    gates = probs_all * hits / picked_sum
    d_probs = hits * (d_gate_dense - jnp.sum(d_gate_dense * gates, axis=1, keepdims=True)) / picked_sum
    return probs_all * (d_probs - jnp.sum(d_probs * probs_all, axis=1, keepdims=True))


def slot_positions(idx_t, first_expert, local_experts, capacity):
    num_dev, _, num_tokens = idx_t.shape
    experts = first_expert + jnp.arange(local_experts, dtype=jnp.int32)
    hits = jnp.sum((idx_t[:, None, :, :] == experts[None, :, None, None]).astype(jnp.float32), axis=2)
    blocks = num_tokens // TOK_BLOCK
    hit_blk = hits.reshape(num_dev, local_experts, blocks, TOK_BLOCK)
    upto = (jnp.arange(TOK_BLOCK)[:, None] <= jnp.arange(TOK_BLOCK)[None, :]).astype(jnp.bfloat16)
    within = jnp.einsum('debt,tu->debu', hit_blk.astype(jnp.bfloat16), upto, preferred_element_type=jnp.float32)
    totals = jnp.sum(hit_blk, axis=-1)
    strict = (jnp.arange(blocks)[:, None] < jnp.arange(blocks)[None, :])
    before = jnp.sum(jnp.where(strict[None, None], totals[:, :, :, None], 0.0), axis=2)
    position = (within + before[..., None] - 1.0).astype(jnp.int32)
    slot_of = jnp.where((hit_blk > 0) & (position < capacity), position, -1)
    begin = jnp.minimum(before.astype(jnp.int32), capacity)
    end = jnp.minimum((before + totals).astype(jnp.int32), capacity)
    win_start = jnp.minimum(begin // ALIGN * ALIGN, capacity - WIN)
    win_count = jnp.maximum((end - win_start + WIN - 1) // WIN, 1)
    return jnp.transpose(slot_of, (0, 2, 1, 3)), win_start, win_count


def expand_routes(idx_t, values_t, first_expert, local_experts):
    num_dev, _, num_tokens = idx_t.shape
    experts = first_expert + jnp.arange(local_experts, dtype=jnp.int32)
    dense = jnp.sum(jnp.where(idx_t[:, None, :, :] == experts[None, :, None, None], values_t[:, None, :, :], 0.0), axis=2)
    return jnp.transpose(dense.reshape(num_dev, local_experts, num_tokens // TOK_BLOCK, TOK_BLOCK), (0, 2, 1, 3))


def gather_kernel(base_ref, start_ref, count_ref, most_ref, x_ref, dy_ref, slot_ref, gate_ref, *rest, blocks, capacity, group, scaled):
    s_ref, dyr_ref = rest[-3:-1] if not scaled else rest[-2:]
    g_ref = None if scaled else rest[-1]
    dev, part = pl.program_id(0), pl.program_id(1)
    experts = group * pl.num_programs(1)
    s_ref[...] = jnp.zeros_like(s_ref)
    dyr_ref[...] = jnp.zeros_like(dyr_ref)
    if g_ref is not None:
        g_ref[...] = jnp.zeros_like(g_ref)
    row_iota = lax.broadcasted_iota(jnp.int32, (WIN, TOK_BLOCK), 0)

    def at(i, blk):
        return (dev * experts + part * group + i) * blocks + blk

    def window(i, blk, first, floor=None):
        slot_row = slot_ref[0, blk, pl.ds(part * group + i, 1), :]
        hit = slot_row == row_iota + first
        if floor is not None:
            hit = hit & (slot_row >= floor)
        gate_row = gate_ref[0, blk, pl.ds(part * group + i, 1), :]
        gate_col = jnp.sum(jnp.where(hit, gate_row, 0.0), axis=1, keepdims=True)
        return jnp.where(hit, 1.0, 0.0).astype(jnp.bfloat16), gate_col

    def deposit(i, first, s_rows, dy_rows, gate_col):
        rows = pl.ds(pl.multiple_of(first, ALIGN), WIN)
        s_ref[i, 0, rows, :] += s_rows.astype(jnp.bfloat16)
        if scaled:
            dyr_ref[i, 0, rows, :] += (dy_rows * gate_col).astype(jnp.bfloat16)
        else:
            dyr_ref[i, 0, rows, :] += dy_rows.astype(jnp.bfloat16)
            g_ref[i, 0, rows, :] += gate_col

    for blk in range(blocks):
        tokens = slice(blk * TOK_BLOCK, (blk + 1) * TOK_BLOCK)
        firsts = [start_ref[at(i, blk)] for i in range(group)]
        parts = [window(i, blk, firsts[i]) for i in range(group)]
        pick = jnp.concatenate([p[0] for p in parts], axis=0)
        s_all = jnp.dot(pick, x_ref[tokens, :], preferred_element_type=jnp.float32)
        dy_all = jnp.dot(pick, dy_ref[tokens, :], preferred_element_type=jnp.float32)
        for i in range(group):
            rows = slice(i * WIN, (i + 1) * WIN)
            deposit(i, firsts[i], s_all[rows], dy_all[rows], parts[i][1])

    @pl.when(most_ref[dev * pl.num_programs(1) + part] > 1)
    def _():
        for i in range(group):
            def per_block(blk, carry):
                def extra(w, inner):
                    floor = start_ref[at(i, blk)] + w * WIN
                    first = jnp.minimum(floor, capacity - WIN)
                    pick, gate_col = window(i, blk, first, floor)
                    tokens = pl.ds(pl.multiple_of(blk * TOK_BLOCK, TOK_BLOCK), TOK_BLOCK)
                    s_rows = jnp.dot(pick, x_ref[tokens, :], preferred_element_type=jnp.float32)
                    dy_rows = jnp.dot(pick, dy_ref[tokens, :], preferred_element_type=jnp.float32)
                    deposit(i, first, s_rows, dy_rows, gate_col)
                    return inner
                return lax.fori_loop(1, count_ref[at(i, blk)], extra, carry)
            lax.fori_loop(0, blocks, per_block, 0)


def gather_slots(base_dev, routes, dev_from, num_dev, x_table, dy_table, filled, total_dev, capacity, scaled, from_all):
    slot_of, win_start, win_count, gate_of = (r[dev_from:dev_from + num_dev] for r in routes)
    _, blocks, experts, _ = slot_of.shape
    width = x_table.shape[1]
    num_tokens = blocks * TOK_BLOCK
    group = 4
    most = jnp.max(win_count.reshape(num_dev, experts // group, group * blocks), axis=2).reshape(-1)

    def table_map(d, p, base_ref, *_):
        return (lax.bitwise_xor(d + dev_from, base_ref[0]) if from_all else 0, 0)

    def route_map(d, p, *_):
        return (d, 0, 0, 0)

    def out_map(d, p, *_):
        return (p, d + dev_from, 0, 0)

    def gate_map(d, p, *_):
        return (p, d, 0, 0)

    rows_shape = jax.ShapeDtypeStruct((experts, total_dev, capacity, width), jnp.bfloat16)
    row_spec = pl.BlockSpec((group, 1, capacity, width), out_map)
    out_shape, out_specs = [rows_shape, rows_shape], [row_spec, row_spec]
    if not scaled:
        out_shape.append(jax.ShapeDtypeStruct((experts, num_dev, capacity, 1), jnp.float32))
        out_specs.append(pl.BlockSpec((group, 1, capacity, 1), gate_map))
    held = () if filled is None else tuple(filled)
    return pl.pallas_call(
        functools.partial(gather_kernel, blocks=blocks, capacity=capacity, group=group, scaled=scaled),
        out_shape=out_shape,
        grid_spec=pltpu.PrefetchScalarGridSpec(
            num_scalar_prefetch=4, grid=(num_dev, experts // group),
            in_specs=[pl.BlockSpec((num_tokens, width), table_map), pl.BlockSpec((num_tokens, width), table_map),
                      pl.BlockSpec((1, blocks, experts, TOK_BLOCK), route_map), pl.BlockSpec((1, blocks, experts, TOK_BLOCK), route_map)]
                     + [pl.BlockSpec(memory_space=pl.ANY)] * len(held),
            out_specs=out_specs),
        input_output_aliases={8 + i: i for i in range(len(held))},
        compiler_params=pltpu.CompilerParams(vmem_limit_bytes=VMEM_MAX, dimension_semantics=('arbitrary', 'arbitrary')),
        cost_estimate=pl.CostEstimate(flops=4 * num_dev * blocks * experts * WIN * TOK_BLOCK * width,
                                      bytes_accessed=4 * num_dev * (num_tokens + experts * capacity) * width, transcendentals=0),
        name='gather_slots',
    )(base_dev, win_start.reshape(-1), win_count.reshape(-1), most, x_table, dy_table, slot_of, gate_of, *held)


def dot_nn(left, right):
    return jnp.dot(left, right, preferred_element_type=jnp.float32)


def dot_nt(left, right):
    return lax.dot_general(left, right, (((1,), (1,)), ((), ())), preferred_element_type=jnp.float32)


def expert_kernel(*refs, own, chunk, held):
    if own:
        s_ref, dy_ref, g_ref, wg_ref, wu_ref, wd_ref = refs[:6]
        hid_ref, dag_ref, dau_ref, do_ref, ds_ref, dgate_ref = refs[6 + held:]
        do_ref[0] = (dy_ref[0].astype(jnp.float32) * g_ref[0]).astype(jnp.bfloat16)
    else:
        s_ref, do_ref, wg_ref, wu_ref, wd_ref = refs[:5]
        hid_ref, dag_ref, dau_ref = refs[5 + held:]
    width = s_ref.shape[-1]
    for c in range(0, width, chunk):
        cols = slice(c, c + chunk)
        act_gate = dot_nn(s_ref[0], wg_ref[0, :, cols])
        act_up = dot_nn(s_ref[0], wu_ref[0, :, cols])
        d_hidden = dot_nt(do_ref[0], wd_ref[0, cols, :])
        sig = jax.nn.sigmoid(act_gate)
        silu = act_gate * sig
        hid_ref[0, :, cols] = (silu * act_up).astype(jnp.bfloat16)
        dau_ref[0, :, cols] = (d_hidden * silu).astype(jnp.bfloat16)
        dag_ref[0, :, cols] = (d_hidden * act_up * (sig * (1.0 + act_gate * (1.0 - sig)))).astype(jnp.bfloat16)
    if own:
        d_gate = None
        for c in range(0, width, chunk):
            cols = slice(c, c + chunk)
            out = dot_nn(hid_ref[0], wd_ref[0, :, cols]).astype(jnp.bfloat16).astype(jnp.float32)
            part = jnp.sum(out * dy_ref[0, :, cols].astype(jnp.float32), axis=1, keepdims=True)
            d_gate = part if d_gate is None else d_gate + part
            ds_ref[0, :, cols] = (dot_nt(dag_ref[0], wg_ref[0, cols, :]) + dot_nt(dau_ref[0], wu_ref[0, cols, :])).astype(jnp.bfloat16)
        dgate_ref[0] = d_gate


def expert_pass(own, tile, first_tile, num_tiles, s_rows, dy_rows, gate_col, w_gate, w_up, w_down, filled):
    experts, rows, width = s_rows.shape
    row_spec = pl.BlockSpec((1, tile, width), lambda e, r: (e, first_tile + r, 0))
    near_spec = pl.BlockSpec((1, tile, width), lambda e, r: (e, r, 0))
    col_spec = pl.BlockSpec((1, tile, 1), lambda e, r: (e, r, 0))
    w_spec = pl.BlockSpec((1, width, width), lambda e, r: (e, 0, 0))
    full = jax.ShapeDtypeStruct((experts, rows, width), jnp.bfloat16)
    out_shape, out_specs = [full] * 3, [row_spec] * 3
    args, in_specs = [s_rows, dy_rows], [row_spec, row_spec]
    aliases = {}
    if own:
        args.append(gate_col)
        in_specs.append(col_spec)
        out_shape += [full, jax.ShapeDtypeStruct((experts, num_tiles * tile, width), jnp.bfloat16),
                      jax.ShapeDtypeStruct((experts, num_tiles * tile, 1), jnp.float32)]
        out_specs += [row_spec, near_spec, col_spec]
        aliases[1] = 3
    args += [w_gate, w_up, w_down]
    in_specs += [w_spec] * 3
    held = () if filled is None else tuple(filled)
    for i, arr in enumerate(held):
        aliases[len(args)] = i
        args.append(arr)
        in_specs.append(pl.BlockSpec(memory_space=pl.ANY))
    units = 6 if own else 3
    return pl.pallas_call(
        functools.partial(expert_kernel, own=own, chunk=min(256, width), held=len(held)),
        out_shape=out_shape, grid=(experts, num_tiles), in_specs=in_specs, out_specs=out_specs,
        input_output_aliases=aliases,
        compiler_params=pltpu.CompilerParams(vmem_limit_bytes=VMEM_MAX, dimension_semantics=('arbitrary', 'arbitrary')),
        cost_estimate=pl.CostEstimate(flops=2 * units * experts * num_tiles * tile * width * width,
                                      bytes_accessed=2 * experts * width * (3 * width + 7 * num_tiles * tile),
                                      transcendentals=experts * num_tiles * tile * width),
        name='expert_own' if own else 'expert_far',
    )(*args)


def combine_kernel(home_ref, start_ref, count_ref, most_ref, ds_ref, dg_ref, slot_ref, *rest, experts, blocks, capacity):
    out_ref, dgt_ref = rest[-2:]
    dev, blk = pl.program_id(0), pl.program_id(1)
    row_iota = lax.broadcasted_iota(jnp.int32, (WIN, TOK_BLOCK), 0)

    def window(e, first, floor=None):
        slot_row = slot_ref[0, 0, e:e + 1, :]
        hit = slot_row == row_iota + first
        if floor is not None:
            hit = hit & (slot_row >= floor)
        rows = pl.ds(pl.multiple_of(first, ALIGN), WIN)
        gate_row = jnp.sum(jnp.where(hit, dg_ref[e, 0, rows, :], 0.0), axis=0, keepdims=True)
        return jnp.where(hit, 1.0, 0.0).astype(jnp.bfloat16), ds_ref[e, 0, rows, :], gate_row

    def spread(pick, rows):
        return lax.dot_general(pick, rows, (((0,), (0,)), ((), ())), preferred_element_type=jnp.float32)

    parts = [window(e, start_ref[(dev * experts + e) * blocks + blk]) for e in range(experts)]
    out_ref[...] = spread(jnp.concatenate([p[0] for p in parts], axis=0), jnp.concatenate([p[1] for p in parts], axis=0))
    for e in range(experts):
        dgt_ref[0, 0, e:e + 1, :] = parts[e][2]

    @pl.when(most_ref[dev * blocks + blk] > 1)
    def _():
        for e in range(experts):
            at = (dev * experts + e) * blocks + blk

            def extra(w, carry):
                floor = start_ref[at] + w * WIN
                pick, rows, gate_row = window(e, jnp.minimum(floor, capacity - WIN), floor)
                out_ref[...] += spread(pick, rows)
                dgt_ref[0, 0, e:e + 1, :] += gate_row
                return carry
            lax.fori_loop(1, count_ref[at], extra, 0)


def combine_slots(home, routes, dev_from, num_dev, total_dev, d_slots, d_gate_slots, filled):
    slot_of, win_start, win_count = (r[dev_from:dev_from + num_dev] for r in routes[:3])
    experts, _, capacity, width = d_slots.shape
    blocks = slot_of.shape[1]
    num_tokens = blocks * TOK_BLOCK
    most = jnp.max(win_count, axis=1).reshape(-1)

    def home_of(d, home_ref):
        return lax.bitwise_xor(d + dev_from, home_ref[0])

    held = () if filled is None else tuple(filled)
    return pl.pallas_call(
        functools.partial(combine_kernel, experts=experts, blocks=blocks, capacity=capacity),
        out_shape=[jax.ShapeDtypeStruct((total_dev * num_tokens, width), jnp.float32),
                   jax.ShapeDtypeStruct((total_dev, blocks, experts, TOK_BLOCK), jnp.float32)],
        grid_spec=pltpu.PrefetchScalarGridSpec(
            num_scalar_prefetch=4, grid=(num_dev, blocks),
            in_specs=[pl.BlockSpec((experts, 1, capacity, width), lambda d, b, *_: (0, d, 0, 0)),
                      pl.BlockSpec((experts, 1, capacity, 1), lambda d, b, *_: (0, d, 0, 0)),
                      pl.BlockSpec((1, 1, experts, TOK_BLOCK), lambda d, b, *_: (d, b, 0, 0))]
                     + [pl.BlockSpec(memory_space=pl.ANY)] * len(held),
            out_specs=[pl.BlockSpec((TOK_BLOCK, width), lambda d, b, home_ref, *_: (home_of(d, home_ref) * blocks + b, 0)),
                       pl.BlockSpec((1, 1, experts, TOK_BLOCK), lambda d, b, home_ref, *_: (home_of(d, home_ref), b, 0, 0))]),
        input_output_aliases={7 + i: i for i in range(len(held))},
        compiler_params=pltpu.CompilerParams(vmem_limit_bytes=VMEM_MAX, dimension_semantics=('arbitrary', 'arbitrary')),
        cost_estimate=pl.CostEstimate(flops=2 * num_dev * blocks * experts * WIN * TOK_BLOCK * width,
                                      bytes_accessed=2 * num_dev * (2 * num_tokens + experts * capacity) * width, transcendentals=0),
        name='combine_slots',
    )(home, win_start.reshape(-1), win_count.reshape(-1), most, d_slots, d_gate_slots, slot_of, *held)


def dense_backward(saved_state, x_rows, dy_rows, d_logits, d_normed2_moe, norm1_gain, norm2_gain, w_qkv, w_attn_out, w_router):
    normed1, attn_pullback, context, h_rows, normed2 = saved_state
    d_w_router = jnp.einsum('td,te->de', normed2, d_logits, preferred_element_type=jnp.float32)
    d_normed2 = d_normed2_moe + jnp.einsum('te,de->td', d_logits, w_router, preferred_element_type=jnp.float32)
    d_h_part, d_norm2_gain = rms_norm_bwd(h_rows, norm2_gain, d_normed2)
    d_h = (dy_rows.astype(jnp.float32) + d_h_part).astype(jnp.bfloat16)
    d_w_attn_out = jnp.einsum('td,te->de', context, d_h, preferred_element_type=jnp.float32)
    d_context = jnp.einsum('te,de->td', d_h, w_attn_out, preferred_element_type=jnp.float32).astype(jnp.bfloat16)
    d_qkv = attn_pullback(d_context)[0].astype(jnp.bfloat16)
    d_w_qkv = jnp.einsum('td,te->de', normed1, d_qkv, preferred_element_type=jnp.float32)
    d_normed1 = jnp.einsum('te,de->td', d_qkv, w_qkv, preferred_element_type=jnp.float32)
    d_x_part, d_norm1_gain = rms_norm_bwd(x_rows, norm1_gain, d_normed1)
    d_x = (d_h.astype(jnp.float32) + d_x_part).astype(jnp.bfloat16)
    return d_x, (d_norm1_gain, d_norm2_gain, d_w_qkv, d_w_attn_out, d_w_router)


def solution(mesh):
    ep_size, dp_size = mesh.shape['ep'], mesh.shape['dp']
    num_dev = ep_size * dp_size
    tok_spec = P(('dp', 'ep'), None, None)
    rep_spec = P()
    exp_spec = P('ep', None, None)
    pair = [(r, r ^ 1) for r in range(ep_size)]

    def local_step(x_tokens, dy_tokens, route_idx, norm1_gain, norm2_gain, w_qkv, w_attn_out, w_router, w_gate, w_up, w_down):
        num_seqs, seq_len, model_width = x_tokens.shape
        num_tokens = num_seqs * seq_len
        top_k = route_idx.shape[-1]
        local_experts = w_gate.shape[0]
        num_experts = local_experts * ep_size
        capacity = capacity_rows(num_tokens, top_k, num_experts)
        x_rows = x_tokens.reshape(num_tokens, model_width)
        dy_rows = dy_tokens.reshape(num_tokens, model_width)
        idx_rows = route_idx.reshape(num_tokens, top_k)
        ep_rank = lax.axis_index('ep')
        me = lax.axis_index('dp') * ep_size + ep_rank
        first_expert = ep_rank * local_experts
        order = jnp.bitwise_xor(me, jnp.arange(num_dev, dtype=jnp.int32))

        idx_wide = lax.all_gather(jnp.concatenate([idx_rows.T] * 4, axis=0), ('dp', 'ep'), axis=0)
        dy_all = lax.all_gather(dy_rows, ('dp', 'ep'), axis=0, tiled=True)
        dy_pair = lax.ppermute(dy_rows, 'ep', pair)
        idx_all = jnp.take(idx_wide[:, :top_k], order, axis=0)
        slot_of, win_start, win_count = slot_positions(idx_all, first_expert, local_experts, capacity)

        normed1 = rms_norm(x_rows, norm1_gain)
        qkv_rows = jnp.dot(normed1, w_qkv, preferred_element_type=jnp.float32)
        context, attn_pullback = jax.vjp(lambda qkv_in: attention_core(qkv_in, num_seqs), qkv_rows)
        h_rows = (x_rows.astype(jnp.float32) + jnp.dot(context, w_attn_out, preferred_element_type=jnp.float32)).astype(jnp.bfloat16)
        normed2 = rms_norm(h_rows, norm2_gain)
        x_pair = lax.ppermute(normed2, 'ep', pair)
        logits = jnp.dot(normed2, w_router, preferred_element_type=jnp.float32)
        probs_all, hits, picked_sum = gate_forward(logits, idx_rows, num_experts)
        gates = probs_all * hits / picked_sum
        gate_t = jnp.sum(jnp.where(choice_mask(idx_rows, num_experts), gates[:, None, :], 0.0), axis=2).T
        gate_pair = lax.ppermute(gate_t, 'ep', pair)
        gate_wide = lax.all_gather(jnp.concatenate([gate_t] * 4, axis=0), ('dp', 'ep'), axis=0)
        normed2_out, _ = lax.optimization_barrier((normed2, dy_all))
        x_all = lax.all_gather(normed2_out, ('dp', 'ep'), axis=0, tiled=True)
        gate_near = expand_routes(idx_all[:2], jnp.stack([gate_t, gate_pair]), first_expert, local_experts)
        gate_far = expand_routes(idx_all[2:], jnp.take(gate_wide[:, :top_k], order[2:], axis=0), first_expert, local_experts)

        near_routes = (slot_of[:2], win_start[:2], win_count[:2], gate_near)
        all_routes = (slot_of, win_start, win_count, jnp.concatenate([jnp.zeros_like(gate_near), gate_far], axis=0))
        gather = functools.partial(gather_slots, me[None], total_dev=num_dev, capacity=capacity)
        s_arr, dy_arr, g0 = gather(near_routes, 0, 1, normed2, dy_rows, None, scaled=False, from_all=False)
        s_arr, dy_arr, g1 = gather(near_routes, 1, 1, x_pair, dy_pair, (s_arr, dy_arr), scaled=False, from_all=False)
        tile = 2 * capacity
        rows_of = lambda a: a.reshape(local_experts, -1, a.shape[-1])
        slots_of = lambda a, n: a.reshape(local_experts, n, capacity, a.shape[-1])
        g_near = rows_of(jnp.concatenate([g0, g1], axis=1))
        hidden, dag, dau, d_out, ds_near, dg_near = expert_pass(True, tile, 0, 1, rows_of(s_arr), rows_of(dy_arr), g_near, w_gate, w_up, w_down, None)
        s_arr, dy_arr, g_x = gather(all_routes, 2, 2, x_all, dy_all, (s_arr, slots_of(d_out, num_dev)), scaled=False, from_all=True)
        hidden, dag, dau, d_out, ds_x, dg_x = expert_pass(True, tile, 1, 1, rows_of(s_arr), rows_of(dy_arr), rows_of(g_x), w_gate, w_up, w_down, (hidden, dag, dau))
        combined = combine_slots(ep_rank[None], all_routes, 2, 2, ep_size, slots_of(ds_x, 2), slots_of(dg_x, 2), None)
        d_tok, d_gate_t = combine_slots(ep_rank[None], all_routes, 0, 2, ep_size, slots_of(ds_near, 2), slots_of(dg_near, 2), combined)
        d_normed2_moe = lax.psum_scatter(d_tok, 'ep', scatter_dimension=0, tiled=True)
        d_gate_blk = lax.all_to_all(d_gate_t, 'ep', 0, 0, tiled=True)
        d_gate_dense = jnp.transpose(d_gate_blk, (1, 3, 0, 2)).reshape(num_tokens, num_experts)
        d_out, _ = lax.optimization_barrier((d_out, d_tok))
        s_arr, dy_arr = gather(all_routes, 4, 4, x_all, dy_all, (s_arr, slots_of(d_out, num_dev)), scaled=True, from_all=True)
        s_all, d_out = rows_of(s_arr), rows_of(dy_arr)
        hidden, dag, dau = expert_pass(False, tile, 2, 2, s_all, d_out, None, w_gate, w_up, w_down, (hidden, dag, dau))
        mm = functools.partial(jnp.einsum, preferred_element_type=jnp.float32)
        d_w_down = mm('ecf,ecd->efd', hidden, d_out)
        d_w_gate = mm('ecd,ecf->edf', s_all, dag)
        d_w_up = mm('ecd,ecf->edf', s_all, dau)

        d_logits = gate_backward(probs_all, hits, picked_sum, d_gate_dense).astype(jnp.bfloat16)
        saved_state = (normed1, attn_pullback, context, h_rows, normed2)
        d_x, dense_grads = dense_backward(saved_state, x_rows, dy_rows, d_logits, d_normed2_moe, norm1_gain, norm2_gain, w_qkv, w_attn_out, w_router)
        dense_grads = lax.psum(dense_grads, ('dp', 'ep'))
        return (d_x.reshape(x_tokens.shape),) + tuple(dense_grads) + (d_w_gate, d_w_up, d_w_down)

    return jax.shard_map(local_step, mesh=mesh,
                         in_specs=(tok_spec, tok_spec, tok_spec, rep_spec, rep_spec, rep_spec, rep_spec, rep_spec, exp_spec, exp_spec, exp_spec),
                         out_specs=(tok_spec, rep_spec, rep_spec, rep_spec, rep_spec, rep_spec, exp_spec, exp_spec, exp_spec),
                         check_vma=False)
```

```python
import functools

import jax
import jax.numpy as jnp
from jax import lax
from jax.experimental import pallas as pl
from jax.experimental.pallas import tpu as pltpu
from jax.sharding import PartitionSpec as P

EPS = 1e-6
HEAD_DIM = 128
ROPE_BASE = 10000.0
TOK_BLOCK = 256
WIN = 64
ALIGN = 16
GROUP = 4
VMEM_MAX = 64 * 1024 * 1024 - 65536


def capacity_rows(num_tokens, top_k, num_experts):
    return 8 * ((5 * num_tokens * top_k + 32 * num_experts - 1) // (32 * num_experts))


def rms_norm(x_rows, gain_vec):
    x_f32 = x_rows.astype(jnp.float32)
    inv_rms = lax.rsqrt(jnp.mean(x_f32 * x_f32, axis=-1, keepdims=True) + EPS)
    return (x_f32 * inv_rms * gain_vec.astype(jnp.float32)).astype(jnp.bfloat16)


def rms_norm_bwd(x_rows, gain_vec, d_out):
    x_f32 = x_rows.astype(jnp.float32)
    inv_rms = lax.rsqrt(jnp.mean(x_f32 * x_f32, axis=-1, keepdims=True) + EPS)
    d_gain = jnp.sum(d_out * x_f32 * inv_rms, axis=0)
    d_scaled = d_out * gain_vec.astype(jnp.float32)
    d_x = inv_rms * d_scaled - x_f32 * inv_rms ** 3 * jnp.mean(d_scaled * x_f32, axis=-1, keepdims=True)
    return d_x, d_gain


def dot_nn(left, right):
    return jnp.dot(left, right, preferred_element_type=jnp.float32)


def dot_nt(left, right):
    return lax.dot_general(left, right, (((1,), (1,)), ((), ())), preferred_element_type=jnp.float32)


def rope_tables(seq_len):
    half_dim = HEAD_DIM // 2
    inv_freq = ROPE_BASE ** (-jnp.arange(half_dim, dtype=jnp.float32) / half_dim)
    angles = jnp.arange(seq_len, dtype=jnp.float32)[:, None] * inv_freq[None, :]
    cos_b, sin_b = jnp.cos(angles), jnp.sin(angles)
    return jnp.concatenate([cos_b, cos_b], axis=1), jnp.concatenate([-sin_b, sin_b], axis=1)


def qkv_kernel(x_ref, gain_ref, w_ref, cos_ref, sin_ref, normed_ref, qkv_ref, *, rotated, chunk):
    x_f32 = x_ref[...].astype(jnp.float32)
    inv_rms = lax.rsqrt(jnp.mean(x_f32 * x_f32, axis=-1, keepdims=True) + EPS)
    normed_ref[...] = (x_f32 * inv_rms * gain_ref[...]).astype(jnp.bfloat16)
    for c in range(0, w_ref.shape[1], chunk):
        acc = dot_nn(normed_ref[...], w_ref[:, c:c + chunk])
        for h in range(0, chunk, HEAD_DIM):
            head = acc[:, h:h + HEAD_DIM]
            if c + h < rotated:
                head = head * cos_ref[...] + pltpu.roll(head, HEAD_DIM // 2, 1) * sin_ref[...]
            qkv_ref[:, c + h:c + h + HEAD_DIM] = head.astype(jnp.bfloat16)


def qkv_project(x_rows, gain_vec, w_qkv, cos_t, sin_t):
    num_tokens, width = x_rows.shape
    seq_len = cos_t.shape[0]
    tile = min(512, seq_len)
    per_seq = seq_len // tile
    row_spec = pl.BlockSpec((tile, width), lambda r: (r, 0))
    table_spec = pl.BlockSpec((tile, HEAD_DIM), lambda r: (lax.rem(r, per_seq), 0))
    return pl.pallas_call(
        functools.partial(qkv_kernel, rotated=2 * width, chunk=256),
        out_shape=[jax.ShapeDtypeStruct((num_tokens, width), jnp.bfloat16), jax.ShapeDtypeStruct((num_tokens, 3 * width), jnp.bfloat16)],
        grid=(num_tokens // tile,),
        in_specs=[row_spec, pl.BlockSpec((1, width), lambda r: (0, 0)), pl.BlockSpec((width, 3 * width), lambda r: (0, 0)), table_spec, table_spec],
        out_specs=[row_spec, pl.BlockSpec((tile, 3 * width), lambda r: (r, 0))],
        compiler_params=pltpu.CompilerParams(vmem_limit_bytes=VMEM_MAX, dimension_semantics=('arbitrary',)),
        cost_estimate=pl.CostEstimate(flops=6 * num_tokens * width * width, bytes_accessed=2 * width * (5 * num_tokens + 3 * width), transcendentals=num_tokens),
        name='qkv_project',
    )(x_rows, gain_vec.astype(jnp.float32)[None, :], w_qkv, cos_t, sin_t)


def attend_kernel(q_ref, k_ref, v_ref, ctx_ref, *, block):
    seq_len = q_ref.shape[0]
    diag = lax.broadcasted_iota(jnp.int32, (block, block), 0) >= lax.broadcasted_iota(jnp.int32, (block, block), 1)
    for start in range(0, seq_len, block):
        stop = start + block
        scores = dot_nt(q_ref[start:stop, :], k_ref[:stop, :]) * HEAD_DIM ** -0.5
        last = jnp.where(diag, scores[:, start:], -1e30)
        scores = last if start == 0 else jnp.concatenate([scores[:, :start], last], axis=1)
        raised = jnp.exp(scores - jnp.max(scores, axis=1, keepdims=True))
        probs = (raised * (1.0 / jnp.sum(raised, axis=1, keepdims=True))).astype(jnp.bfloat16)
        ctx_ref[start:stop, :] = dot_nn(probs, v_ref[:stop, :]).astype(jnp.bfloat16)


def head_spec(seq_len, offset):
    return pl.BlockSpec((seq_len, HEAD_DIM), lambda s, h: (s, h + offset))


def attend(qkv_rot, num_seqs):
    num_tokens, width = qkv_rot.shape[0], qkv_rot.shape[1] // 3
    seq_len, heads = num_tokens // num_seqs, width // HEAD_DIM
    return pl.pallas_call(
        functools.partial(attend_kernel, block=min(256, seq_len)),
        out_shape=jax.ShapeDtypeStruct((num_tokens, width), jnp.bfloat16),
        grid=(num_seqs, heads),
        in_specs=[head_spec(seq_len, 0), head_spec(seq_len, heads), head_spec(seq_len, 2 * heads)],
        out_specs=head_spec(seq_len, 0),
        compiler_params=pltpu.CompilerParams(vmem_limit_bytes=VMEM_MAX, dimension_semantics=('arbitrary', 'arbitrary')),
        cost_estimate=pl.CostEstimate(flops=4 * num_tokens * seq_len * width, bytes_accessed=8 * num_tokens * width, transcendentals=num_tokens * seq_len * heads),
        name='attend',
    )(qkv_rot, qkv_rot, qkv_rot)


def attend_back_kernel(q_ref, k_ref, v_ref, dctx_ref, cos_ref, sin_ref, out_ref, stage, d_key, d_val, sems, *, block, heads):
    seq, head = pl.program_id(0), pl.program_id(1)
    step = seq * heads + head
    slot = lax.rem(step, 2)
    seq_len = q_ref.shape[0]
    scale = HEAD_DIM ** -0.5
    causal = lax.broadcasted_iota(jnp.int32, (block, block), 0) <= lax.broadcasted_iota(jnp.int32, (block, block), 1)

    def copies(at_step, at_slot):
        at_seq, at_head = at_step // heads, lax.rem(at_step, heads)
        rows = pl.ds(pl.multiple_of(at_seq * seq_len, seq_len), seq_len)
        return [pltpu.make_async_copy(stage.at[at_slot, i],
                                      out_ref.at[rows, pl.ds(pl.multiple_of((at_head + i * heads) * HEAD_DIM, HEAD_DIM), HEAD_DIM)],
                                      sems.at[at_slot, i]) for i in range(3)]

    @pl.when(step >= 2)
    def _():
        for copy in copies(step - 2, slot):
            copy.wait()

    def unrotate(grad):
        grad = grad.astype(jnp.bfloat16).astype(jnp.float32)
        return lambda cos, sin: (grad * cos + pltpu.roll(grad * sin, HEAD_DIM // 2, 1)).astype(jnp.bfloat16)

    key_t = jnp.transpose(k_ref[...])
    for start in range(0, seq_len, block):
        stop = start + block
        query, d_ctx = q_ref[start:stop, :], dctx_ref[start:stop, :]
        scores = dot_nt(k_ref[:stop, :], query) * scale
        last = jnp.where(causal, scores[start:, :], -1e30)
        scores = last if start == 0 else jnp.concatenate([scores[:start, :], last], axis=0)
        raised = jnp.exp(scores - jnp.max(scores, axis=0, keepdims=True))
        probs = raised * (1.0 / jnp.sum(raised, axis=0, keepdims=True))
        d_probs = dot_nt(v_ref[:stop, :], d_ctx).astype(jnp.bfloat16).astype(jnp.float32)
        mean_d = jnp.sum(d_probs * probs, axis=0, keepdims=True)
        d_scores = (probs * (d_probs - mean_d) * scale).astype(jnp.bfloat16)
        d_v = dot_nn(probs.astype(jnp.bfloat16), d_ctx)
        d_k = dot_nn(d_scores, query)
        if start == 0:
            d_val[:stop, :] = d_v
            d_key[:stop, :] = d_k
        else:
            d_val[:start, :] += d_v[:start]
            d_key[:start, :] += d_k[:start]
            d_val[start:stop, :] = d_v[start:]
            d_key[start:stop, :] = d_k[start:]
        d_q = jnp.transpose(dot_nn(key_t[:, :stop], d_scores))
        stage[slot, 0, start:stop, :] = unrotate(d_q)(cos_ref[start:stop, :], sin_ref[start:stop, :])
    stage[slot, 1] = unrotate(d_key[...])(cos_ref[...], sin_ref[...])
    stage[slot, 2] = d_val[...].astype(jnp.bfloat16)
    for copy in copies(step, slot):
        copy.start()

    @pl.when(step == pl.num_programs(0) * heads - 1)
    def _():
        for copy in copies(step - 1, 1 - slot):
            copy.wait()
        for copy in copies(step, slot):
            copy.wait()


def attend_back(qkv_rot, d_context, cos_t, sin_t, num_seqs):
    num_tokens, width = d_context.shape
    seq_len, heads = num_tokens // num_seqs, width // HEAD_DIM
    table_spec = pl.BlockSpec((seq_len, HEAD_DIM), lambda s, h: (0, 0))
    return pl.pallas_call(
        functools.partial(attend_back_kernel, block=min(256, seq_len), heads=heads),
        out_shape=jax.ShapeDtypeStruct((num_tokens, 3 * width), jnp.bfloat16),
        grid=(num_seqs, heads),
        in_specs=[head_spec(seq_len, 0), head_spec(seq_len, heads), head_spec(seq_len, 2 * heads), head_spec(seq_len, 0), table_spec, table_spec],
        out_specs=pl.BlockSpec(memory_space=pl.ANY),
        scratch_shapes=[pltpu.VMEM((2, 3, seq_len, HEAD_DIM), jnp.bfloat16), pltpu.VMEM((seq_len, HEAD_DIM), jnp.float32),
                        pltpu.VMEM((seq_len, HEAD_DIM), jnp.float32), pltpu.SemaphoreType.DMA((2, 3))],
        compiler_params=pltpu.CompilerParams(vmem_limit_bytes=VMEM_MAX, dimension_semantics=('arbitrary', 'arbitrary')),
        cost_estimate=pl.CostEstimate(flops=10 * num_tokens * seq_len * width, bytes_accessed=14 * num_tokens * width, transcendentals=num_tokens * seq_len * heads),
        name='attend_back',
    )(qkv_rot, qkv_rot, qkv_rot, d_context, cos_t, sin_t)


def choice_mask(idx_rows, num_experts):
    return (idx_rows[:, :, None] == jnp.arange(num_experts, dtype=jnp.int32)[None, None, :])


def gate_forward(logits, idx_rows, num_experts):
    probs_all = jax.nn.softmax(logits, axis=-1)
    hits = jnp.sum(choice_mask(idx_rows, num_experts).astype(jnp.float32), axis=1)
    picked_sum = jnp.sum(probs_all * hits, axis=1, keepdims=True)
    return probs_all, hits, picked_sum


def gate_backward(probs_all, hits, picked_sum, d_gate_dense):
    gates = probs_all * hits / picked_sum
    d_probs = hits * (d_gate_dense - jnp.sum(d_gate_dense * gates, axis=1, keepdims=True)) / picked_sum
    return probs_all * (d_probs - jnp.sum(d_probs * probs_all, axis=1, keepdims=True))


def slot_positions(idx_t, first_expert, local_experts, capacity):
    num_dev, _, num_tokens = idx_t.shape
    experts = first_expert + jnp.arange(local_experts, dtype=jnp.int32)
    hits = jnp.sum((idx_t[:, None, :, :] == experts[None, :, None, None]).astype(jnp.float32), axis=2)
    blocks = num_tokens // TOK_BLOCK
    hit_blk = hits.reshape(num_dev, local_experts, blocks, TOK_BLOCK)
    upto = (jnp.arange(TOK_BLOCK)[:, None] <= jnp.arange(TOK_BLOCK)[None, :]).astype(jnp.bfloat16)
    within = jnp.einsum('debt,tu->debu', hit_blk.astype(jnp.bfloat16), upto, preferred_element_type=jnp.float32)
    totals = jnp.sum(hit_blk, axis=-1)
    strict = (jnp.arange(blocks)[:, None] < jnp.arange(blocks)[None, :])
    before = jnp.sum(jnp.where(strict[None, None], totals[:, :, :, None], 0.0), axis=2)
    position = (within + before[..., None] - 1.0).astype(jnp.int32)
    slot_of = jnp.where((hit_blk > 0) & (position < capacity), position, -1)
    begin = jnp.minimum(before.astype(jnp.int32), capacity)
    end = jnp.minimum((before + totals).astype(jnp.int32), capacity)
    win_start = jnp.minimum(begin // ALIGN * ALIGN, capacity - WIN)
    win_count = jnp.maximum((end - win_start + WIN - 1) // WIN, 1)
    most_group = jnp.max(win_count.reshape(num_dev, local_experts // GROUP, GROUP * blocks), axis=2)
    most_block = jnp.max(win_count, axis=1)
    return jnp.transpose(slot_of, (0, 2, 1, 3)), win_start.reshape(-1), win_count.reshape(-1), most_group.reshape(-1), most_block.reshape(-1)


def expand_routes(idx_t, values_t, first_expert, local_experts):
    num_dev, _, num_tokens = idx_t.shape
    experts = first_expert + jnp.arange(local_experts, dtype=jnp.int32)
    dense = jnp.sum(jnp.where(idx_t[:, None, :, :] == experts[None, :, None, None], values_t[:, None, :, :], 0.0), axis=2)
    return jnp.transpose(dense.reshape(num_dev, local_experts, num_tokens // TOK_BLOCK, TOK_BLOCK), (0, 2, 1, 3))


def gather_kernel(base_ref, start_ref, count_ref, most_ref, x_ref, dy_ref, slot_ref, gate_ref, *rest, blocks, capacity, group, scaled, dev_from):
    s_ref, dyr_ref = rest[-2:] if scaled else rest[-3:-1]
    g_ref = None if scaled else rest[-1]
    dev, part = pl.program_id(0) + dev_from, pl.program_id(1)
    experts = group * pl.num_programs(1)
    s_ref[...] = jnp.zeros_like(s_ref)
    dyr_ref[...] = jnp.zeros_like(dyr_ref)
    if g_ref is not None:
        g_ref[...] = jnp.zeros_like(g_ref)
    row_iota = lax.broadcasted_iota(jnp.int32, (WIN, TOK_BLOCK), 0)

    def at(i, blk):
        return (dev * experts + part * group + i) * blocks + blk

    def window(i, blk, first, floor=None):
        slot_row = slot_ref[0, blk, pl.ds(part * group + i, 1), :]
        hit = slot_row == row_iota + first
        if floor is not None:
            hit = hit & (slot_row >= floor)
        gate_row = gate_ref[0, blk, pl.ds(part * group + i, 1), :]
        gate_col = jnp.sum(jnp.where(hit, gate_row, 0.0), axis=1, keepdims=True)
        return jnp.where(hit, 1.0, 0.0).astype(jnp.bfloat16), gate_col

    def deposit(i, first, s_rows, dy_rows, gate_col):
        rows = pl.ds(pl.multiple_of(first, ALIGN), WIN)
        s_ref[i, 0, rows, :] += s_rows.astype(jnp.bfloat16)
        if scaled:
            dyr_ref[i, 0, rows, :] += (dy_rows * gate_col).astype(jnp.bfloat16)
        else:
            dyr_ref[i, 0, rows, :] += dy_rows.astype(jnp.bfloat16)
            g_ref[i, 0, rows, :] += gate_col

    for blk in range(blocks):
        tokens = slice(blk * TOK_BLOCK, (blk + 1) * TOK_BLOCK)
        firsts = [start_ref[at(i, blk)] for i in range(group)]
        parts = [window(i, blk, firsts[i]) for i in range(group)]
        pick = jnp.concatenate([p[0] for p in parts], axis=0)
        s_all = jnp.dot(pick, x_ref[tokens, :], preferred_element_type=jnp.float32)
        dy_all = jnp.dot(pick, dy_ref[tokens, :], preferred_element_type=jnp.float32)
        for i in range(group):
            rows = slice(i * WIN, (i + 1) * WIN)
            deposit(i, firsts[i], s_all[rows], dy_all[rows], parts[i][1])

    @pl.when(most_ref[dev * pl.num_programs(1) + part] > 1)
    def _():
        for i in range(group):
            def per_block(blk, carry):
                def extra(w, inner):
                    floor = start_ref[at(i, blk)] + w * WIN
                    first = jnp.minimum(floor, capacity - WIN)
                    pick, gate_col = window(i, blk, first, floor)
                    tokens = pl.ds(pl.multiple_of(blk * TOK_BLOCK, TOK_BLOCK), TOK_BLOCK)
                    s_rows = jnp.dot(pick, x_ref[tokens, :], preferred_element_type=jnp.float32)
                    dy_rows = jnp.dot(pick, dy_ref[tokens, :], preferred_element_type=jnp.float32)
                    deposit(i, first, s_rows, dy_rows, gate_col)
                    return inner

                return lax.fori_loop(1, count_ref[at(i, blk)], extra, carry)

            lax.fori_loop(0, blocks, per_block, 0)


def gather_slots(base_dev, routes, dev_from, num_dev, gate_of, x_table, dy_table, filled, own_dev, capacity, scaled, from_all):
    slot_of, win_start, win_count, most, _ = routes
    total_dev, blocks, experts, _ = slot_of.shape
    width = x_table.shape[1]
    num_tokens = blocks * TOK_BLOCK
    group = GROUP

    def table_map(d, p, base_ref, *_):
        return (lax.bitwise_xor(d + dev_from, base_ref[0]) if from_all else 0, 0)

    def slot_map(d, p, *_):
        return (d + dev_from, 0, 0, 0)

    def gate_map(d, p, *_):
        return (d, 0, 0, 0)

    def out_map(d, p, *_):
        return (p, d + dev_from, 0, 0)

    rows_shape = jax.ShapeDtypeStruct((experts, total_dev, capacity, width), jnp.bfloat16)
    row_spec = pl.BlockSpec((group, 1, capacity, width), out_map)
    out_shape, out_specs = [rows_shape, rows_shape], [row_spec, row_spec]
    if not scaled:
        out_shape.append(jax.ShapeDtypeStruct((experts, own_dev, capacity, 1), jnp.float32))
        out_specs.append(pl.BlockSpec((group, 1, capacity, 1), out_map))
    held = () if filled is None else tuple(filled)
    route_block = (1, blocks, experts, TOK_BLOCK)
    return pl.pallas_call(
        functools.partial(gather_kernel, blocks=blocks, capacity=capacity, group=group, scaled=scaled, dev_from=dev_from),
        out_shape=out_shape,
        grid_spec=pltpu.PrefetchScalarGridSpec(
            num_scalar_prefetch=4, grid=(num_dev, experts // group),
            in_specs=[pl.BlockSpec((num_tokens, width), table_map), pl.BlockSpec((num_tokens, width), table_map),
                      pl.BlockSpec(route_block, slot_map), pl.BlockSpec(route_block, gate_map)]
                     + [pl.BlockSpec(memory_space=pl.ANY)] * len(held),
            out_specs=out_specs),
        input_output_aliases={8 + i: i for i in range(len(held))},
        compiler_params=pltpu.CompilerParams(vmem_limit_bytes=VMEM_MAX, dimension_semantics=('arbitrary', 'arbitrary')),
        cost_estimate=pl.CostEstimate(flops=4 * num_dev * blocks * experts * WIN * TOK_BLOCK * width,
                                      bytes_accessed=4 * num_dev * (num_tokens + experts * capacity) * width, transcendentals=0),
        name='gather_slots',
    )(base_dev, win_start, win_count, most, x_table, dy_table, slot_of, gate_of, *held)


def expert_kernel(*refs, own, chunk, held):
    if own:
        s_ref, dy_ref, g_ref, wg_ref, wu_ref, wd_ref = refs[:6]
        hid_ref, dag_ref, dau_ref, do_ref, ds_ref, dgate_ref = refs[6 + held:]
        do_ref[0] = (dy_ref[0].astype(jnp.float32) * g_ref[0]).astype(jnp.bfloat16)
    else:
        s_ref, do_ref, wg_ref, wu_ref, wd_ref = refs[:5]
        hid_ref, dag_ref, dau_ref = refs[5 + held:]
    width = s_ref.shape[-1]
    for c in range(0, width, chunk):
        cols = slice(c, c + chunk)
        act_gate = dot_nn(s_ref[0], wg_ref[0, :, cols])
        act_up = dot_nn(s_ref[0], wu_ref[0, :, cols])
        d_hidden = dot_nt(do_ref[0], wd_ref[0, cols, :])
        sig = jax.nn.sigmoid(act_gate)
        silu = act_gate * sig
        hid_ref[0, :, cols] = (silu * act_up).astype(jnp.bfloat16)
        dau_ref[0, :, cols] = (d_hidden * silu).astype(jnp.bfloat16)
        dag_ref[0, :, cols] = (d_hidden * act_up * (sig * (1.0 + act_gate * (1.0 - sig)))).astype(jnp.bfloat16)
    if own:
        d_gate = None
        for c in range(0, width, chunk):
            cols = slice(c, c + chunk)
            out = dot_nn(hid_ref[0], wd_ref[0, :, cols]).astype(jnp.bfloat16).astype(jnp.float32)
            part = jnp.sum(out * dy_ref[0, :, cols].astype(jnp.float32), axis=1, keepdims=True)
            d_gate = part if d_gate is None else d_gate + part
            ds_ref[0, :, cols] = (dot_nt(dag_ref[0], wg_ref[0, cols, :]) + dot_nt(dau_ref[0], wu_ref[0, cols, :])).astype(jnp.bfloat16)
        dgate_ref[0] = d_gate


def expert_pass(own, tile, first_tile, num_tiles, s_rows, dy_rows, gate_col, w_gate, w_up, w_down, filled):
    experts, rows, width = s_rows.shape
    row_spec = pl.BlockSpec((1, tile, width), lambda e, r: (e, first_tile + r, 0))
    near_spec = pl.BlockSpec((1, tile, width), lambda e, r: (e, r, 0))
    col_spec = pl.BlockSpec((1, tile, 1), lambda e, r: (e, first_tile + r, 0))
    near_col_spec = pl.BlockSpec((1, tile, 1), lambda e, r: (e, r, 0))
    w_spec = pl.BlockSpec((1, width, width), lambda e, r: (e, 0, 0))
    full = jax.ShapeDtypeStruct((experts, rows, width), jnp.bfloat16)
    out_shape, out_specs = [full] * 3, [row_spec] * 3
    args, in_specs = [s_rows, dy_rows], [row_spec, row_spec]
    aliases = {}
    if own:
        args.append(gate_col)
        in_specs.append(col_spec)
        out_shape += [full, jax.ShapeDtypeStruct((experts, num_tiles * tile, width), jnp.bfloat16),
                      jax.ShapeDtypeStruct((experts, num_tiles * tile, 1), jnp.float32)]
        out_specs += [row_spec, near_spec, near_col_spec]
        aliases[1] = 3
    args += [w_gate, w_up, w_down]
    in_specs += [w_spec] * 3
    held = () if filled is None else tuple(filled)
    for i, arr in enumerate(held):
        aliases[len(args)] = i
        args.append(arr)
        in_specs.append(pl.BlockSpec(memory_space=pl.ANY))
    units = 6 if own else 3
    return pl.pallas_call(
        functools.partial(expert_kernel, own=own, chunk=min(256, width), held=len(held)),
        out_shape=out_shape, grid=(experts, num_tiles), in_specs=in_specs, out_specs=out_specs,
        input_output_aliases=aliases,
        compiler_params=pltpu.CompilerParams(vmem_limit_bytes=VMEM_MAX, dimension_semantics=('arbitrary', 'arbitrary')),
        cost_estimate=pl.CostEstimate(flops=2 * units * experts * num_tiles * tile * width * width,
                                      bytes_accessed=2 * experts * width * (3 * width + 7 * num_tiles * tile),
                                      transcendentals=experts * num_tiles * tile * width),
        name='expert_own' if own else 'expert_far',
    )(*args)


def combine_kernel(home_ref, start_ref, count_ref, most_ref, ds_ref, dg_ref, slot_ref, *rest, experts, blocks, capacity, dev_from):
    out_ref, dgt_ref = rest[-2:]
    dev, blk = pl.program_id(0) + dev_from, pl.program_id(1)
    row_iota = lax.broadcasted_iota(jnp.int32, (WIN, TOK_BLOCK), 0)

    def window(e, first, floor=None):
        slot_row = slot_ref[0, 0, e:e + 1, :]
        hit = slot_row == row_iota + first
        if floor is not None:
            hit = hit & (slot_row >= floor)
        rows = pl.ds(pl.multiple_of(first, ALIGN), WIN)
        gate_row = jnp.sum(jnp.where(hit, dg_ref[e, 0, rows, :], 0.0), axis=0, keepdims=True)
        return jnp.where(hit, 1.0, 0.0).astype(jnp.bfloat16), ds_ref[e, 0, rows, :], gate_row

    def spread(pick, rows):
        return lax.dot_general(pick, rows, (((0,), (0,)), ((), ())), preferred_element_type=jnp.float32)

    parts = [window(e, start_ref[(dev * experts + e) * blocks + blk]) for e in range(experts)]
    out_ref[...] = spread(jnp.concatenate([p[0] for p in parts], axis=0), jnp.concatenate([p[1] for p in parts], axis=0))
    for e in range(experts):
        dgt_ref[0, 0, e:e + 1, :] = parts[e][2]

    @pl.when(most_ref[dev * blocks + blk] > 1)
    def _():
        for e in range(experts):
            at = (dev * experts + e) * blocks + blk

            def extra(w, carry):
                floor = start_ref[at] + w * WIN
                pick, rows, gate_row = window(e, jnp.minimum(floor, capacity - WIN), floor)
                out_ref[...] += spread(pick, rows)
                dgt_ref[0, 0, e:e + 1, :] += gate_row
                return carry

            lax.fori_loop(1, count_ref[at], extra, 0)


def combine_slots(home, routes, dev_from, num_dev, total_dev, d_slots, d_gate_slots, filled):
    slot_of, win_start, win_count, _, most = routes
    experts, _, capacity, width = d_slots.shape
    blocks = slot_of.shape[1]
    num_tokens = blocks * TOK_BLOCK

    def home_of(d, home_ref):
        return lax.bitwise_xor(d + dev_from, home_ref[0])

    held = () if filled is None else tuple(filled)
    return pl.pallas_call(
        functools.partial(combine_kernel, experts=experts, blocks=blocks, capacity=capacity, dev_from=dev_from),
        out_shape=[jax.ShapeDtypeStruct((total_dev * num_tokens, width), jnp.float32),
                   jax.ShapeDtypeStruct((total_dev, blocks, experts, TOK_BLOCK), jnp.float32)],
        grid_spec=pltpu.PrefetchScalarGridSpec(
            num_scalar_prefetch=4, grid=(num_dev, blocks),
            in_specs=[pl.BlockSpec((experts, 1, capacity, width), lambda d, b, *_: (0, d, 0, 0)),
                      pl.BlockSpec((experts, 1, capacity, 1), lambda d, b, *_: (0, d, 0, 0)),
                      pl.BlockSpec((1, 1, experts, TOK_BLOCK), lambda d, b, *_: (d + dev_from, b, 0, 0))]
                     + [pl.BlockSpec(memory_space=pl.ANY)] * len(held),
            out_specs=[pl.BlockSpec((TOK_BLOCK, width), lambda d, b, home_ref, *_: (home_of(d, home_ref) * blocks + b, 0)),
                       pl.BlockSpec((1, 1, experts, TOK_BLOCK), lambda d, b, home_ref, *_: (home_of(d, home_ref), b, 0, 0))]),
        input_output_aliases={7 + i: i for i in range(len(held))},
        compiler_params=pltpu.CompilerParams(vmem_limit_bytes=VMEM_MAX, dimension_semantics=('arbitrary', 'arbitrary')),
        cost_estimate=pl.CostEstimate(flops=2 * num_dev * blocks * experts * WIN * TOK_BLOCK * width,
                                      bytes_accessed=2 * num_dev * (2 * num_tokens + experts * capacity) * width, transcendentals=0),
        name='combine_slots',
    )(home, win_start, win_count, most, d_slots, d_gate_slots, slot_of, *held)


def dense_backward(saved_state, x_rows, dy_rows, d_logits, d_normed2_moe, norm1_gain, norm2_gain, w_qkv, w_attn_out, w_router):
    normed1, qkv_rot, context, h_rows, normed2, cos_t, sin_t, num_seqs = saved_state
    d_w_router = jnp.einsum('td,te->de', normed2, d_logits, preferred_element_type=jnp.float32)
    d_normed2 = d_normed2_moe + jnp.einsum('te,de->td', d_logits, w_router, preferred_element_type=jnp.float32)
    d_h_part, d_norm2_gain = rms_norm_bwd(h_rows, norm2_gain, d_normed2)
    d_h = (dy_rows.astype(jnp.float32) + d_h_part).astype(jnp.bfloat16)
    d_w_attn_out = jnp.einsum('td,te->de', context, d_h, preferred_element_type=jnp.float32)
    d_context = jnp.einsum('te,de->td', d_h, w_attn_out, preferred_element_type=jnp.float32).astype(jnp.bfloat16)
    d_qkv = attend_back(qkv_rot, d_context, cos_t, sin_t, num_seqs)
    d_w_qkv = jnp.einsum('td,te->de', normed1, d_qkv, preferred_element_type=jnp.float32)
    d_normed1 = jnp.einsum('te,de->td', d_qkv, w_qkv, preferred_element_type=jnp.float32)
    d_x_part, d_norm1_gain = rms_norm_bwd(x_rows, norm1_gain, d_normed1)
    d_x = (d_h.astype(jnp.float32) + d_x_part).astype(jnp.bfloat16)
    small = jnp.concatenate([d_w_router, d_norm1_gain[:, None], d_norm2_gain[:, None]], axis=1)
    return d_x, d_qkv, (d_w_qkv, d_w_attn_out, small)


def solution(mesh):
    ep_size, dp_size = mesh.shape['ep'], mesh.shape['dp']
    num_dev = ep_size * dp_size
    tok_spec = P(('dp', 'ep'), None, None)
    rep_spec = P()
    exp_spec = P('ep', None, None)

    def swap(value, distance):
        return lax.ppermute(value, 'ep', [(r, r ^ distance) for r in range(ep_size)])

    def spread_routes(value):
        near = jnp.stack([value, swap(value, 1)])
        row = [near, jnp.stack([swap(value, 2), swap(value, 3)])]
        far = lax.ppermute(jnp.concatenate(row, axis=0), 'dp', [(r, r ^ 1) for r in range(dp_size)])
        return row + [far]

    def local_step(x_tokens, dy_tokens, route_idx, norm1_gain, norm2_gain, w_qkv, w_attn_out, w_router, w_gate, w_up, w_down):
        num_seqs, seq_len, model_width = x_tokens.shape
        num_tokens = num_seqs * seq_len
        top_k = route_idx.shape[-1]
        local_experts = w_gate.shape[0]
        num_experts = local_experts * ep_size
        capacity = capacity_rows(num_tokens, top_k, num_experts)
        x_rows = x_tokens.reshape(num_tokens, model_width)
        dy_rows = dy_tokens.reshape(num_tokens, model_width)
        idx_rows = route_idx.reshape(num_tokens, top_k)
        ep_rank = lax.axis_index('ep')
        me = lax.axis_index('dp') * ep_size + ep_rank
        first_expert = ep_rank * local_experts

        dy_all = lax.all_gather(dy_rows, ('dp', 'ep'), axis=0, tiled=True)
        idx_parts = spread_routes(idx_rows.T)
        dy_pair = swap(dy_rows, 1)
        routes = slot_positions(jnp.concatenate(idx_parts, axis=0), first_expert, local_experts, capacity)

        cos_t, sin_t = rope_tables(seq_len)
        normed1, qkv_rot = qkv_project(x_rows, norm1_gain, w_qkv, cos_t, sin_t)
        qkv_rot, routes = lax.optimization_barrier((qkv_rot, routes))
        context = attend(qkv_rot, num_seqs)
        h_rows = (x_rows.astype(jnp.float32) + jnp.dot(context, w_attn_out, preferred_element_type=jnp.float32)).astype(jnp.bfloat16)
        normed2 = rms_norm(h_rows, norm2_gain)
        x_pair = swap(normed2, 1)
        logits = jnp.dot(normed2, w_router, preferred_element_type=jnp.float32)
        probs_all, hits, picked_sum = gate_forward(logits, idx_rows, num_experts)
        gates = probs_all * hits / picked_sum
        gate_t = jnp.sum(jnp.where(choice_mask(idx_rows, num_experts), gates[:, None, :], 0.0), axis=2).T
        x_all = lax.all_gather(normed2, ('dp', 'ep'), axis=0, tiled=True)
        gate_near, gate_x, gate_far = (expand_routes(i, g, first_expert, local_experts) for i, g in zip(idx_parts, spread_routes(gate_t)))

        gather = functools.partial(gather_slots, me[None], routes, own_dev=ep_size, capacity=capacity)
        rows_of = lambda a: a.reshape(local_experts, -1, a.shape[-1])
        slots_of = lambda a, n: a.reshape(local_experts, n, capacity, a.shape[-1])
        combine = functools.partial(combine_slots, ep_rank[None], routes, total_dev=ep_size)
        weights = (w_gate, w_up, w_down)
        tile = 2 * capacity
        arrays = gather(0, 1, gate_near[:1], normed2, dy_rows, None, scaled=False, from_all=False)
        s_arr, dy_arr, g_arr = gather(1, 1, gate_near[1:], x_pair, dy_pair, arrays, scaled=False, from_all=False)
        hidden, dag, dau, d_out, ds_near, dg_near = expert_pass(True, tile, 0, 1, rows_of(s_arr), rows_of(dy_arr), rows_of(g_arr), *weights, None)
        combined = combine(0, 2, d_slots=slots_of(ds_near, 2), d_gate_slots=slots_of(dg_near, 2), filled=None)
        s_arr, dy_arr, g_arr = gather(2, 2, gate_x, x_all, dy_all, (s_arr, slots_of(d_out, num_dev), g_arr), scaled=False, from_all=True)
        hidden, dag, dau, d_out, ds_x, dg_x = expert_pass(True, tile, 1, 1, rows_of(s_arr), rows_of(dy_arr), rows_of(g_arr), *weights, (hidden, dag, dau))
        d_tok, d_gate_t = combine(2, 2, d_slots=slots_of(ds_x, 2), d_gate_slots=slots_of(dg_x, 2), filled=combined)
        d_normed2_moe = lax.psum_scatter(d_tok, 'ep', scatter_dimension=0, tiled=True)
        d_gate_blk = lax.all_to_all(d_gate_t, 'ep', 0, 0, tiled=True)
        d_gate_dense = jnp.transpose(d_gate_blk, (1, 3, 0, 2)).reshape(num_tokens, num_experts)
        d_out, _ = lax.optimization_barrier((d_out, d_tok))
        s_arr, dy_arr = gather(4, 4, gate_far, x_all, dy_all, (s_arr, slots_of(d_out, num_dev)), scaled=True, from_all=True)
        s_all, d_out = rows_of(s_arr), rows_of(dy_arr)
        hidden, dag, dau = expert_pass(False, tile, 2, 2, s_all, d_out, None, *weights, (hidden, dag, dau))
        mm = functools.partial(jnp.einsum, preferred_element_type=jnp.float32)
        d_w_down = mm('ecf,ecd->efd', hidden, d_out)

        d_logits = gate_backward(probs_all, hits, picked_sum, d_gate_dense).astype(jnp.bfloat16)
        saved_state = (normed1, qkv_rot, context, h_rows, normed2, cos_t, sin_t, num_seqs)
        d_x, d_qkv, dense_grads = dense_backward(saved_state, x_rows, dy_rows, d_logits, d_normed2_moe, norm1_gain, norm2_gain, w_qkv, w_attn_out, w_router)
        d_w_qkv, d_w_attn_out, small = lax.psum(dense_grads, ('dp', 'ep'))
        s_all, dag, dau, _ = lax.optimization_barrier((s_all, dag, dau, d_qkv))
        d_w_gate = mm('ecd,ecf->edf', s_all, dag)
        d_w_up = mm('ecd,ecf->edf', s_all, dau)
        return (d_x.reshape(x_tokens.shape), small[:, num_experts], small[:, num_experts + 1], d_w_qkv, d_w_attn_out, small[:, :num_experts],
                d_w_gate, d_w_up, d_w_down)

    return jax.shard_map(local_step, mesh=mesh,
                         in_specs=(tok_spec, tok_spec, tok_spec, rep_spec, rep_spec, rep_spec, rep_spec, rep_spec, exp_spec, exp_spec, exp_spec),
                         out_specs=(tok_spec, rep_spec, rep_spec, rep_spec, rep_spec, rep_spec, exp_spec, exp_spec, exp_spec),
                         check_vma=False)
```

```python
import functools

import jax
import jax.numpy as jnp
from jax import lax
from jax.experimental import pallas as pl
from jax.experimental.pallas import tpu as pltpu
from jax.sharding import PartitionSpec as P

EPS = 1e-6
HEAD_DIM = 128
ROPE_BASE = 10000.0
TOK_BLOCK = 256
WIN = 64
ALIGN = 16
GROUP = 4
VMEM_MAX = 64 * 1024 * 1024 - 65536


def capacity_rows(num_tokens, top_k, num_experts):
    return 8 * ((5 * num_tokens * top_k + 32 * num_experts - 1) // (32 * num_experts))


def rms_norm(x_rows, gain_vec):
    x_f32 = x_rows.astype(jnp.float32)
    inv_rms = lax.rsqrt(jnp.mean(x_f32 * x_f32, axis=-1, keepdims=True) + EPS)
    return (x_f32 * inv_rms * gain_vec.astype(jnp.float32)).astype(jnp.bfloat16)


def rms_norm_bwd(x_rows, gain_vec, d_out):
    x_f32 = x_rows.astype(jnp.float32)
    inv_rms = lax.rsqrt(jnp.mean(x_f32 * x_f32, axis=-1, keepdims=True) + EPS)
    d_gain = jnp.sum(d_out * x_f32 * inv_rms, axis=0)
    d_scaled = d_out * gain_vec.astype(jnp.float32)
    d_x = inv_rms * d_scaled - x_f32 * inv_rms ** 3 * jnp.mean(d_scaled * x_f32, axis=-1, keepdims=True)
    return d_x, d_gain


def dot_nn(left, right):
    return jnp.dot(left, right, preferred_element_type=jnp.float32)


def dot_nt(left, right):
    return lax.dot_general(left, right, (((1,), (1,)), ((), ())), preferred_element_type=jnp.float32)


def rope_tables(seq_len):
    half_dim = HEAD_DIM // 2
    inv_freq = ROPE_BASE ** (-jnp.arange(half_dim, dtype=jnp.float32) / half_dim)
    angles = jnp.arange(seq_len, dtype=jnp.float32)[:, None] * inv_freq[None, :]
    cos_b, sin_b = jnp.cos(angles), jnp.sin(angles)
    return jnp.concatenate([cos_b, cos_b], axis=1), jnp.concatenate([-sin_b, sin_b], axis=1)


def qkv_kernel(x_ref, gain_ref, w_ref, cos_ref, sin_ref, normed_ref, qkv_ref, *, rotated, chunk):
    x_f32 = x_ref[...].astype(jnp.float32)
    inv_rms = lax.rsqrt(jnp.mean(x_f32 * x_f32, axis=-1, keepdims=True) + EPS)
    normed_ref[...] = (x_f32 * inv_rms * gain_ref[...]).astype(jnp.bfloat16)
    for c in range(0, w_ref.shape[1], chunk):
        acc = dot_nn(normed_ref[...], w_ref[:, c:c + chunk])
        for h in range(0, chunk, HEAD_DIM):
            head = acc[:, h:h + HEAD_DIM]
            if c + h < rotated:
                head = head * cos_ref[...] + pltpu.roll(head, HEAD_DIM // 2, 1) * sin_ref[...]
            qkv_ref[:, c + h:c + h + HEAD_DIM] = head.astype(jnp.bfloat16)


def qkv_project(x_rows, gain_vec, w_qkv, cos_t, sin_t):
    num_tokens, width = x_rows.shape
    seq_len = cos_t.shape[0]
    tile = min(512, seq_len)
    per_seq = seq_len // tile
    row_spec = pl.BlockSpec((tile, width), lambda r: (r, 0))
    table_spec = pl.BlockSpec((tile, HEAD_DIM), lambda r: (lax.rem(r, per_seq), 0))
    return pl.pallas_call(
        functools.partial(qkv_kernel, rotated=2 * width, chunk=256),
        out_shape=[jax.ShapeDtypeStruct((num_tokens, width), jnp.bfloat16), jax.ShapeDtypeStruct((num_tokens, 3 * width), jnp.bfloat16)],
        grid=(num_tokens // tile,),
        in_specs=[row_spec, pl.BlockSpec((1, width), lambda r: (0, 0)), pl.BlockSpec((width, 3 * width), lambda r: (0, 0)), table_spec, table_spec],
        out_specs=[row_spec, pl.BlockSpec((tile, 3 * width), lambda r: (r, 0))],
        compiler_params=pltpu.CompilerParams(vmem_limit_bytes=VMEM_MAX, dimension_semantics=('arbitrary',)),
        cost_estimate=pl.CostEstimate(flops=6 * num_tokens * width * width, bytes_accessed=2 * width * (5 * num_tokens + 3 * width), transcendentals=num_tokens),
        name='qkv_project',
    )(x_rows, gain_vec.astype(jnp.float32)[None, :], w_qkv, cos_t, sin_t)


def attend_kernel(q_all, k_all, v_all, ctx_all, *, block):
    seq_len = q_all.shape[0]
    diag = lax.broadcasted_iota(jnp.int32, (block, block), 0) >= lax.broadcasted_iota(jnp.int32, (block, block), 1)
    for first in range(0, q_all.shape[1], HEAD_DIM):
        q_ref, k_ref, v_ref, ctx_ref = (ref.at[:, first:first + HEAD_DIM] for ref in (q_all, k_all, v_all, ctx_all))
        for start in range(0, seq_len, block):
            stop = start + block
            scores = dot_nt(q_ref[start:stop, :], k_ref[:stop, :]) * HEAD_DIM ** -0.5
            last = jnp.where(diag, scores[:, start:], -1e30)
            scores = last if start == 0 else jnp.concatenate([scores[:, :start], last], axis=1)
            raised = jnp.exp(scores - jnp.max(scores, axis=1, keepdims=True))
            probs = (raised * (1.0 / jnp.sum(raised, axis=1, keepdims=True))).astype(jnp.bfloat16)
            ctx_ref[start:stop, :] = dot_nn(probs, v_ref[:stop, :]).astype(jnp.bfloat16)


def head_spec(seq_len, offset, heads=1):
    return pl.BlockSpec((seq_len, heads * HEAD_DIM), lambda s, h: (s, h + offset // heads))


def attend(qkv_rot, num_seqs):
    num_tokens, width = qkv_rot.shape[0], qkv_rot.shape[1] // 3
    seq_len, heads = num_tokens // num_seqs, width // HEAD_DIM
    return pl.pallas_call(
        functools.partial(attend_kernel, block=min(256, seq_len)),
        out_shape=jax.ShapeDtypeStruct((num_tokens, width), jnp.bfloat16),
        grid=(num_seqs, heads // 2),
        in_specs=[head_spec(seq_len, 0, 2), head_spec(seq_len, heads, 2), head_spec(seq_len, 2 * heads, 2)],
        out_specs=head_spec(seq_len, 0, 2),
        compiler_params=pltpu.CompilerParams(vmem_limit_bytes=VMEM_MAX, dimension_semantics=('arbitrary', 'arbitrary')),
        cost_estimate=pl.CostEstimate(flops=4 * num_tokens * seq_len * width, bytes_accessed=8 * num_tokens * width, transcendentals=num_tokens * seq_len * heads),
        name='attend',
    )(qkv_rot, qkv_rot, qkv_rot)


def attend_back_kernel(q_ref, k_ref, v_ref, dctx_ref, cos_ref, sin_ref, out_ref, stage, d_key, d_val, sems, *, block, heads):
    seq, head = pl.program_id(0), pl.program_id(1)
    step = seq * heads + head
    slot = lax.rem(step, 2)
    seq_len = q_ref.shape[0]
    scale = HEAD_DIM ** -0.5
    causal = lax.broadcasted_iota(jnp.int32, (block, block), 0) <= lax.broadcasted_iota(jnp.int32, (block, block), 1)

    def copies(at_step, at_slot):
        at_seq, at_head = at_step // heads, lax.rem(at_step, heads)
        rows = pl.ds(pl.multiple_of(at_seq * seq_len, seq_len), seq_len)
        return [pltpu.make_async_copy(stage.at[at_slot, i],
                                      out_ref.at[rows, pl.ds(pl.multiple_of((at_head + i * heads) * HEAD_DIM, HEAD_DIM), HEAD_DIM)],
                                      sems.at[at_slot, i]) for i in range(3)]

    @pl.when(step >= 2)
    def _():
        for copy in copies(step - 2, slot):
            copy.wait()

    def unrotate(grad):
        grad = grad.astype(jnp.bfloat16).astype(jnp.float32)
        return lambda cos, sin: (grad * cos + pltpu.roll(grad * sin, HEAD_DIM // 2, 1)).astype(jnp.bfloat16)

    key_t = jnp.transpose(k_ref[...])
    for start in range(0, seq_len, block):
        stop = start + block
        query, d_ctx = q_ref[start:stop, :], dctx_ref[start:stop, :]
        scores = dot_nt(k_ref[:stop, :], query) * scale
        last = jnp.where(causal, scores[start:, :], -1e30)
        scores = last if start == 0 else jnp.concatenate([scores[:start, :], last], axis=0)
        raised = jnp.exp(scores - jnp.max(scores, axis=0, keepdims=True))
        probs = raised * (1.0 / jnp.sum(raised, axis=0, keepdims=True))
        d_probs = dot_nt(v_ref[:stop, :], d_ctx).astype(jnp.bfloat16).astype(jnp.float32)
        mean_d = jnp.sum(d_probs * probs, axis=0, keepdims=True)
        d_scores = (probs * (d_probs - mean_d) * scale).astype(jnp.bfloat16)
        d_v = dot_nn(probs.astype(jnp.bfloat16), d_ctx)
        d_k = dot_nn(d_scores, query)
        if start == 0:
            d_val[:stop, :] = d_v
            d_key[:stop, :] = d_k
        else:
            d_val[:start, :] += d_v[:start]
            d_key[:start, :] += d_k[:start]
            d_val[start:stop, :] = d_v[start:]
            d_key[start:stop, :] = d_k[start:]
        d_q = jnp.transpose(dot_nn(key_t[:, :stop], d_scores))
        stage[slot, 0, start:stop, :] = unrotate(d_q)(cos_ref[start:stop, :], sin_ref[start:stop, :])
    stage[slot, 1] = unrotate(d_key[...])(cos_ref[...], sin_ref[...])
    stage[slot, 2] = d_val[...].astype(jnp.bfloat16)
    for copy in copies(step, slot):
        copy.start()

    @pl.when(step == pl.num_programs(0) * heads - 1)
    def _():
        for copy in copies(step - 1, 1 - slot):
            copy.wait()
        for copy in copies(step, slot):
            copy.wait()


def attend_back(qkv_rot, d_context, cos_t, sin_t, num_seqs):
    num_tokens, width = d_context.shape
    seq_len, heads = num_tokens // num_seqs, width // HEAD_DIM
    table_spec = pl.BlockSpec((seq_len, HEAD_DIM), lambda s, h: (0, 0))
    return pl.pallas_call(
        functools.partial(attend_back_kernel, block=min(256, seq_len), heads=heads),
        out_shape=jax.ShapeDtypeStruct((num_tokens, 3 * width), jnp.bfloat16),
        grid=(num_seqs, heads),
        in_specs=[head_spec(seq_len, 0), head_spec(seq_len, heads), head_spec(seq_len, 2 * heads), head_spec(seq_len, 0), table_spec, table_spec],
        out_specs=pl.BlockSpec(memory_space=pl.ANY),
        scratch_shapes=[pltpu.VMEM((2, 3, seq_len, HEAD_DIM), jnp.bfloat16), pltpu.VMEM((seq_len, HEAD_DIM), jnp.float32),
                        pltpu.VMEM((seq_len, HEAD_DIM), jnp.float32), pltpu.SemaphoreType.DMA((2, 3))],
        compiler_params=pltpu.CompilerParams(vmem_limit_bytes=VMEM_MAX, dimension_semantics=('arbitrary', 'arbitrary')),
        cost_estimate=pl.CostEstimate(flops=10 * num_tokens * seq_len * width, bytes_accessed=14 * num_tokens * width, transcendentals=num_tokens * seq_len * heads),
        name='attend_back',
    )(qkv_rot, qkv_rot, qkv_rot, d_context, cos_t, sin_t)


def input_grad_kernel(dqkv_ref, w_ref, x_ref, gain_ref, dh_ref, dx_ref, dgain_ref):
    d_out = dot_nt(dqkv_ref[...], w_ref[...])
    x_f32 = x_ref[...].astype(jnp.float32)
    inv_rms = lax.rsqrt(jnp.mean(x_f32 * x_f32, axis=-1, keepdims=True) + EPS)
    part = jnp.sum(d_out * x_f32 * inv_rms, axis=0, keepdims=True)

    @pl.when(pl.program_id(0) == 0)
    def _():
        dgain_ref[...] = jnp.zeros_like(dgain_ref)

    dgain_ref[...] += part
    d_scaled = d_out * gain_ref[...]
    d_x = inv_rms * d_scaled - x_f32 * (inv_rms * inv_rms * inv_rms) * jnp.mean(d_scaled * x_f32, axis=-1, keepdims=True)
    dx_ref[...] = (dh_ref[...].astype(jnp.float32) + d_x).astype(jnp.bfloat16)


def input_grad(d_qkv, w_qkv, x_rows, gain_vec, d_h):
    num_tokens, width = x_rows.shape
    tile = min(512, num_tokens)
    row_spec = pl.BlockSpec((tile, width), lambda r: (r, 0))
    gain_spec = pl.BlockSpec((1, width), lambda r: (0, 0))
    return pl.pallas_call(
        input_grad_kernel,
        out_shape=[jax.ShapeDtypeStruct((num_tokens, width), jnp.bfloat16), jax.ShapeDtypeStruct((1, width), jnp.float32)],
        grid=(num_tokens // tile,),
        in_specs=[pl.BlockSpec((tile, 3 * width), lambda r: (r, 0)), pl.BlockSpec((width, 3 * width), lambda r: (0, 0)), row_spec, gain_spec, row_spec],
        out_specs=[row_spec, gain_spec],
        compiler_params=pltpu.CompilerParams(vmem_limit_bytes=VMEM_MAX, dimension_semantics=('arbitrary',)),
        cost_estimate=pl.CostEstimate(flops=6 * num_tokens * width * width, bytes_accessed=2 * width * (6 * num_tokens + 3 * width), transcendentals=num_tokens),
        name='input_grad',
    )(d_qkv, w_qkv, x_rows, gain_vec.astype(jnp.float32)[None, :], d_h)


def choice_mask(idx_rows, num_experts):
    return (idx_rows[:, :, None] == jnp.arange(num_experts, dtype=jnp.int32)[None, None, :])


def gate_forward(logits, idx_rows, num_experts):
    probs_all = jax.nn.softmax(logits, axis=-1)
    hits = jnp.sum(choice_mask(idx_rows, num_experts).astype(jnp.float32), axis=1)
    picked_sum = jnp.sum(probs_all * hits, axis=1, keepdims=True)
    return probs_all, hits, picked_sum


def gate_backward(probs_all, hits, picked_sum, d_gate_dense):
    gates = probs_all * hits / picked_sum
    d_probs = hits * (d_gate_dense - jnp.sum(d_gate_dense * gates, axis=1, keepdims=True)) / picked_sum
    return probs_all * (d_probs - jnp.sum(d_probs * probs_all, axis=1, keepdims=True))


def slot_positions(idx_t, first_expert, local_experts, capacity):
    num_dev, _, num_tokens = idx_t.shape
    experts = first_expert + jnp.arange(local_experts, dtype=jnp.int32)
    hits = jnp.sum((idx_t[:, None, :, :] == experts[None, :, None, None]).astype(jnp.float32), axis=2)
    blocks = num_tokens // TOK_BLOCK
    hit_blk = hits.reshape(num_dev, local_experts, blocks, TOK_BLOCK)
    upto = (jnp.arange(TOK_BLOCK)[:, None] <= jnp.arange(TOK_BLOCK)[None, :]).astype(jnp.bfloat16)
    within = jnp.einsum('debt,tu->debu', hit_blk.astype(jnp.bfloat16), upto, preferred_element_type=jnp.float32)
    totals = jnp.sum(hit_blk, axis=-1)
    strict = (jnp.arange(blocks)[:, None] < jnp.arange(blocks)[None, :])
    before = jnp.sum(jnp.where(strict[None, None], totals[:, :, :, None], 0.0), axis=2)
    position = (within + before[..., None] - 1.0).astype(jnp.int32)
    slot_of = jnp.where((hit_blk > 0) & (position < capacity), position, -1)
    begin = jnp.minimum(before.astype(jnp.int32), capacity)
    end = jnp.minimum((before + totals).astype(jnp.int32), capacity)
    win_start = jnp.minimum(begin // ALIGN * ALIGN, capacity - WIN)
    win_count = jnp.maximum((end - win_start + WIN - 1) // WIN, 1)
    filled = jnp.max(end, axis=2)
    most_group = jnp.max(win_count.reshape(num_dev, local_experts // GROUP, GROUP * blocks), axis=2)
    most_block = jnp.max(win_count, axis=1)
    return jnp.transpose(slot_of, (0, 2, 1, 3)), begin.reshape(-1), win_count.reshape(-1), most_group.reshape(-1), most_block.reshape(-1), filled.reshape(-1)


def expand_routes(idx_t, values_t, first_expert, local_experts):
    num_dev, _, num_tokens = idx_t.shape
    experts = first_expert + jnp.arange(local_experts, dtype=jnp.int32)
    dense = jnp.sum(jnp.where(idx_t[:, None, :, :] == experts[None, :, None, None], values_t[:, None, :, :], 0.0), axis=2)
    return jnp.transpose(dense.reshape(num_dev, local_experts, num_tokens // TOK_BLOCK, TOK_BLOCK), (0, 2, 1, 3))


def window_start(begin, capacity):
    return jnp.minimum(lax.div(begin, ALIGN) * ALIGN, capacity - WIN)


def gather_kernel(base_ref, begin_ref, count_ref, most_ref, fill_ref, x_ref, dy_ref, slot_ref, gate_ref, *rest, blocks, capacity, group, scaled, dev_from):
    s_ref, dyr_ref = rest[-2:] if scaled else rest[-3:-1]
    g_ref = None if scaled else rest[-1]
    dev, part = pl.program_id(0) + dev_from, pl.program_id(1)
    experts = group * pl.num_programs(1)
    overflow = most_ref[dev * pl.num_programs(1) + part] > 1

    @pl.when(overflow)
    def _():
        s_ref[...] = jnp.zeros_like(s_ref)
        dyr_ref[...] = jnp.zeros_like(dyr_ref)

    if g_ref is not None:
        g_ref[...] = jnp.zeros_like(g_ref)
    row_iota = lax.broadcasted_iota(jnp.int32, (WIN, TOK_BLOCK), 0)
    line_iota = lax.broadcasted_iota(jnp.int32, (WIN, x_ref.shape[1]), 0)

    def at(i, blk):
        return (dev * experts + part * group + i) * blocks + blk

    def window(i, blk, first, floor=None):
        slot_row = slot_ref[0, blk, pl.ds(part * group + i, 1), :]
        hit = slot_row == row_iota + first
        if floor is not None:
            hit = hit & (slot_row >= floor)
        gate_row = gate_ref[0, blk, pl.ds(part * group + i, 1), :]
        gate_col = jnp.sum(jnp.where(hit, gate_row, 0.0), axis=1, keepdims=True)
        return jnp.where(hit, 1.0, 0.0).astype(jnp.bfloat16), gate_col

    def deposit(i, first, s_rows, dy_rows, gate_col, begin=None):
        rows = pl.ds(pl.multiple_of(first, ALIGN), WIN)
        s_rows = s_rows.astype(jnp.bfloat16)
        dy_rows = (dy_rows * gate_col if scaled else dy_rows).astype(jnp.bfloat16)
        if begin is None:
            s_ref[i, 0, rows, :] += s_rows
            dyr_ref[i, 0, rows, :] += dy_rows
        else:
            earlier = line_iota < begin - first
            s_ref[i, 0, rows, :] = jnp.where(earlier, s_ref[i, 0, rows, :], s_rows)
            dyr_ref[i, 0, rows, :] = jnp.where(earlier, dyr_ref[i, 0, rows, :], dy_rows)
        if not scaled:
            g_ref[i, 0, rows, :] += gate_col

    for blk in range(blocks):
        tokens = slice(blk * TOK_BLOCK, (blk + 1) * TOK_BLOCK)
        begins = [begin_ref[at(i, blk)] for i in range(group)]
        firsts = [window_start(begin, capacity) for begin in begins]
        parts = [window(i, blk, firsts[i]) for i in range(group)]
        pick = jnp.concatenate([p[0] for p in parts], axis=0)
        s_all = jnp.dot(pick, x_ref[tokens, :], preferred_element_type=jnp.float32)
        dy_all = jnp.dot(pick, dy_ref[tokens, :], preferred_element_type=jnp.float32)
        for i in range(group):
            rows = slice(i * WIN, (i + 1) * WIN)
            deposit(i, firsts[i], s_all[rows], dy_all[rows], parts[i][1], begins[i])

    for i in range(group):
        def blank(step, carry):
            rows = pl.ds(pl.multiple_of(step * ALIGN, ALIGN), ALIGN)
            s_ref[i, 0, rows, :] = jnp.zeros((ALIGN, s_ref.shape[-1]), jnp.bfloat16)
            dyr_ref[i, 0, rows, :] = jnp.zeros((ALIGN, s_ref.shape[-1]), jnp.bfloat16)
            return carry

        lax.fori_loop(lax.div(fill_ref[dev * experts + part * group + i] + ALIGN - 1, ALIGN), capacity // ALIGN, blank, 0)

    @pl.when(overflow)
    def _():
        for i in range(group):
            def per_block(blk, carry):
                def extra(w, inner):
                    floor = window_start(begin_ref[at(i, blk)], capacity) + w * WIN
                    first = jnp.minimum(floor, capacity - WIN)
                    pick, gate_col = window(i, blk, first, floor)
                    tokens = pl.ds(pl.multiple_of(blk * TOK_BLOCK, TOK_BLOCK), TOK_BLOCK)
                    s_rows = jnp.dot(pick, x_ref[tokens, :], preferred_element_type=jnp.float32)
                    dy_rows = jnp.dot(pick, dy_ref[tokens, :], preferred_element_type=jnp.float32)
                    deposit(i, first, s_rows, dy_rows, gate_col)
                    return inner

                return lax.fori_loop(1, count_ref[at(i, blk)], extra, carry)

            lax.fori_loop(0, blocks, per_block, 0)


def gather_slots(base_dev, routes, dev_from, num_dev, gate_of, x_table, dy_table, filled, own_dev, capacity, scaled, from_all):
    slot_of, begin, win_count, most, _, fill = routes
    total_dev, blocks, experts, _ = slot_of.shape
    width = x_table.shape[1]
    num_tokens = blocks * TOK_BLOCK
    group = GROUP

    def table_map(d, p, base_ref, *_):
        return (lax.bitwise_xor(d + dev_from, base_ref[0]) if from_all else 0, 0)

    def slot_map(d, p, *_):
        return (d + dev_from, 0, 0, 0)

    def gate_map(d, p, *_):
        return (d, 0, 0, 0)

    def out_map(d, p, *_):
        return (p, d + dev_from, 0, 0)

    rows_shape = jax.ShapeDtypeStruct((experts, total_dev, capacity, width), jnp.bfloat16)
    row_spec = pl.BlockSpec((group, 1, capacity, width), out_map)
    out_shape, out_specs = [rows_shape, rows_shape], [row_spec, row_spec]
    if not scaled:
        out_shape.append(jax.ShapeDtypeStruct((experts, own_dev, capacity, 1), jnp.float32))
        out_specs.append(pl.BlockSpec((group, 1, capacity, 1), out_map))
    held = () if filled is None else tuple(filled)
    route_block = (1, blocks, experts, TOK_BLOCK)
    return pl.pallas_call(
        functools.partial(gather_kernel, blocks=blocks, capacity=capacity, group=group, scaled=scaled, dev_from=dev_from),
        out_shape=out_shape,
        grid_spec=pltpu.PrefetchScalarGridSpec(
            num_scalar_prefetch=5, grid=(num_dev, experts // group),
            in_specs=[pl.BlockSpec((num_tokens, width), table_map), pl.BlockSpec((num_tokens, width), table_map),
                      pl.BlockSpec(route_block, slot_map), pl.BlockSpec(route_block, gate_map)]
                     + [pl.BlockSpec(memory_space=pl.ANY)] * len(held),
            out_specs=out_specs),
        input_output_aliases={9 + i: i for i in range(len(held))},
        compiler_params=pltpu.CompilerParams(vmem_limit_bytes=VMEM_MAX, dimension_semantics=('arbitrary', 'arbitrary')),
        cost_estimate=pl.CostEstimate(flops=4 * num_dev * blocks * experts * WIN * TOK_BLOCK * width,
                                      bytes_accessed=4 * num_dev * (num_tokens + experts * capacity) * width, transcendentals=0),
        name='gather_slots',
    )(base_dev, begin, win_count, most, fill, x_table, dy_table, slot_of, gate_of, *held)


def expert_kernel(*refs, own, chunk, held):
    if own:
        s_ref, dy_ref, g_ref, wg_ref, wu_ref, wd_ref = refs[:6]
        hid_ref, dag_ref, dau_ref, do_ref, ds_ref, dgate_ref = refs[6 + held:]
        do_ref[0] = (dy_ref[0].astype(jnp.float32) * g_ref[0]).astype(jnp.bfloat16)
    else:
        s_ref, do_ref, wg_ref, wu_ref, wd_ref = refs[:5]
        hid_ref, dag_ref, dau_ref = refs[5 + held:]
    width = s_ref.shape[-1]
    for c in range(0, width, chunk):
        cols = slice(c, c + chunk)
        act_gate = dot_nn(s_ref[0], wg_ref[0, :, cols])
        act_up = dot_nn(s_ref[0], wu_ref[0, :, cols])
        d_hidden = dot_nt(do_ref[0], wd_ref[0, cols, :])
        sig = jax.nn.sigmoid(act_gate)
        silu = act_gate * sig
        hid_ref[0, :, cols] = (silu * act_up).astype(jnp.bfloat16)
        dau_ref[0, :, cols] = (d_hidden * silu).astype(jnp.bfloat16)
        dag_ref[0, :, cols] = (d_hidden * act_up * (sig * (1.0 + act_gate * (1.0 - sig)))).astype(jnp.bfloat16)
    if own:
        d_gate = None
        for c in range(0, width, chunk):
            cols = slice(c, c + chunk)
            out = dot_nn(hid_ref[0], wd_ref[0, :, cols]).astype(jnp.bfloat16).astype(jnp.float32)
            part = jnp.sum(out * dy_ref[0, :, cols].astype(jnp.float32), axis=1, keepdims=True)
            d_gate = part if d_gate is None else d_gate + part
            ds_ref[0, :, cols] = (dot_nt(dag_ref[0], wg_ref[0, cols, :]) + dot_nt(dau_ref[0], wu_ref[0, cols, :])).astype(jnp.bfloat16)
        dgate_ref[0] = d_gate


def expert_pass(own, tile, first_tile, num_tiles, s_rows, dy_rows, gate_col, w_gate, w_up, w_down, filled):
    experts, rows, width = s_rows.shape
    row_spec = pl.BlockSpec((1, tile, width), lambda e, r: (e, first_tile + r, 0))
    near_spec = pl.BlockSpec((1, tile, width), lambda e, r: (e, r, 0))
    col_spec = pl.BlockSpec((1, tile, 1), lambda e, r: (e, first_tile + r, 0))
    near_col_spec = pl.BlockSpec((1, tile, 1), lambda e, r: (e, r, 0))
    w_spec = pl.BlockSpec((1, width, width), lambda e, r: (e, 0, 0))
    full = jax.ShapeDtypeStruct((experts, rows, width), jnp.bfloat16)
    out_shape, out_specs = [full] * 3, [row_spec] * 3
    args, in_specs = [s_rows, dy_rows], [row_spec, row_spec]
    aliases = {}
    if own:
        args.append(gate_col)
        in_specs.append(col_spec)
        out_shape += [full, jax.ShapeDtypeStruct((experts, num_tiles * tile, width), jnp.bfloat16),
                      jax.ShapeDtypeStruct((experts, num_tiles * tile, 1), jnp.float32)]
        out_specs += [row_spec, near_spec, near_col_spec]
        aliases[1] = 3
    args += [w_gate, w_up, w_down]
    in_specs += [w_spec] * 3
    held = () if filled is None else tuple(filled)
    for i, arr in enumerate(held):
        aliases[len(args)] = i
        args.append(arr)
        in_specs.append(pl.BlockSpec(memory_space=pl.ANY))
    units = 6 if own else 3
    return pl.pallas_call(
        functools.partial(expert_kernel, own=own, chunk=min(256, width), held=len(held)),
        out_shape=out_shape, grid=(experts, num_tiles), in_specs=in_specs, out_specs=out_specs,
        input_output_aliases=aliases,
        compiler_params=pltpu.CompilerParams(vmem_limit_bytes=VMEM_MAX, dimension_semantics=('arbitrary', 'arbitrary')),
        cost_estimate=pl.CostEstimate(flops=2 * units * experts * num_tiles * tile * width * width,
                                      bytes_accessed=2 * experts * width * (3 * width + 7 * num_tiles * tile),
                                      transcendentals=experts * num_tiles * tile * width),
        name='expert_own' if own else 'expert_far',
    )(*args)


def weight_grad_kernel(*refs, count):
    left_ref, rights, outs = refs[0], refs[1:1 + count], refs[1 + count:]
    for right_ref, out_ref in zip(rights, outs):
        out_ref[0] = lax.dot_general(left_ref[0], right_ref[0], (((0,), (0,)), ((), ())), preferred_element_type=jnp.float32)


def weight_grads(left, *rights):
    experts, rows, width = left.shape
    count = len(rights)
    row_spec = pl.BlockSpec((1, rows, width), lambda e: (e, 0, 0))
    out_spec = pl.BlockSpec((1, width, width), lambda e: (e, 0, 0))
    return pl.pallas_call(
        functools.partial(weight_grad_kernel, count=count),
        out_shape=[jax.ShapeDtypeStruct((experts, width, width), jnp.float32)] * count,
        grid=(experts,), in_specs=[row_spec] * (1 + count), out_specs=[out_spec] * count,
        compiler_params=pltpu.CompilerParams(vmem_limit_bytes=VMEM_MAX, dimension_semantics=('arbitrary',)),
        cost_estimate=pl.CostEstimate(flops=2 * count * experts * rows * width * width,
                                      bytes_accessed=experts * width * (2 * (1 + count) * rows + 4 * count * width), transcendentals=0),
        name='weight_grads',
    )(left, *rights)


def combine_kernel(home_ref, begin_ref, count_ref, most_ref, ds_ref, dg_ref, slot_ref, *rest, experts, blocks, capacity, dev_from):
    out_ref, dgt_ref = rest[-2:]
    dev, blk = pl.program_id(0) + dev_from, pl.program_id(1)
    row_iota = lax.broadcasted_iota(jnp.int32, (WIN, TOK_BLOCK), 0)

    def window(e, first, floor=None):
        slot_row = slot_ref[0, 0, e:e + 1, :]
        hit = slot_row == row_iota + first
        if floor is not None:
            hit = hit & (slot_row >= floor)
        rows = pl.ds(pl.multiple_of(first, ALIGN), WIN)
        gate_row = jnp.sum(jnp.where(hit, dg_ref[e, 0, rows, :], 0.0), axis=0, keepdims=True)
        return jnp.where(hit, 1.0, 0.0).astype(jnp.bfloat16), ds_ref[e, 0, rows, :], gate_row

    def spread(pick, rows):
        return lax.dot_general(pick, rows, (((0,), (0,)), ((), ())), preferred_element_type=jnp.float32)

    parts = [window(e, window_start(begin_ref[(dev * experts + e) * blocks + blk], capacity)) for e in range(experts)]
    out_ref[...] = spread(jnp.concatenate([p[0] for p in parts], axis=0), jnp.concatenate([p[1] for p in parts], axis=0))
    for e in range(experts):
        dgt_ref[0, 0, e:e + 1, :] = parts[e][2]

    @pl.when(most_ref[dev * blocks + blk] > 1)
    def _():
        for e in range(experts):
            at = (dev * experts + e) * blocks + blk

            def extra(w, carry):
                floor = window_start(begin_ref[at], capacity) + w * WIN
                pick, rows, gate_row = window(e, jnp.minimum(floor, capacity - WIN), floor)
                out_ref[...] += spread(pick, rows)
                dgt_ref[0, 0, e:e + 1, :] += gate_row
                return carry

            lax.fori_loop(1, count_ref[at], extra, 0)


def combine_slots(home, routes, dev_from, num_dev, total_dev, d_slots, d_gate_slots, filled):
    slot_of, begin, win_count, _, most, _ = routes
    experts, _, capacity, width = d_slots.shape
    blocks = slot_of.shape[1]
    num_tokens = blocks * TOK_BLOCK

    def home_of(d, home_ref):
        return lax.bitwise_xor(d + dev_from, home_ref[0])

    held = () if filled is None else tuple(filled)
    return pl.pallas_call(
        functools.partial(combine_kernel, experts=experts, blocks=blocks, capacity=capacity, dev_from=dev_from),
        out_shape=[jax.ShapeDtypeStruct((total_dev * num_tokens, width), jnp.float32),
                   jax.ShapeDtypeStruct((total_dev, blocks, experts, TOK_BLOCK), jnp.float32)],
        grid_spec=pltpu.PrefetchScalarGridSpec(
            num_scalar_prefetch=4, grid=(num_dev, blocks),
            in_specs=[pl.BlockSpec((experts, 1, capacity, width), lambda d, b, *_: (0, d, 0, 0)),
                      pl.BlockSpec((experts, 1, capacity, 1), lambda d, b, *_: (0, d, 0, 0)),
                      pl.BlockSpec((1, 1, experts, TOK_BLOCK), lambda d, b, *_: (d + dev_from, b, 0, 0))]
                     + [pl.BlockSpec(memory_space=pl.ANY)] * len(held),
            out_specs=[pl.BlockSpec((TOK_BLOCK, width), lambda d, b, home_ref, *_: (home_of(d, home_ref) * blocks + b, 0)),
                       pl.BlockSpec((1, 1, experts, TOK_BLOCK), lambda d, b, home_ref, *_: (home_of(d, home_ref), b, 0, 0))]),
        input_output_aliases={7 + i: i for i in range(len(held))},
        compiler_params=pltpu.CompilerParams(vmem_limit_bytes=VMEM_MAX, dimension_semantics=('arbitrary', 'arbitrary')),
        cost_estimate=pl.CostEstimate(flops=2 * num_dev * blocks * experts * WIN * TOK_BLOCK * width,
                                      bytes_accessed=2 * num_dev * (2 * num_tokens + experts * capacity) * width, transcendentals=0),
        name='combine_slots',
    )(home, begin, win_count, most, d_slots, d_gate_slots, slot_of, *held)


def dense_backward(saved_state, x_rows, dy_rows, d_logits, d_normed2_moe, norm1_gain, norm2_gain, w_qkv, w_attn_out, w_router):
    normed1, qkv_rot, context, h_rows, normed2, cos_t, sin_t, num_seqs = saved_state
    d_w_router = jnp.einsum('td,te->de', normed2, d_logits, preferred_element_type=jnp.float32)
    d_normed2 = d_normed2_moe + jnp.einsum('te,de->td', d_logits, w_router, preferred_element_type=jnp.float32)
    d_h_part, d_norm2_gain = rms_norm_bwd(h_rows, norm2_gain, d_normed2)
    d_h = (dy_rows.astype(jnp.float32) + d_h_part).astype(jnp.bfloat16)
    d_w_attn_out = jnp.einsum('td,te->de', context, d_h, preferred_element_type=jnp.float32)
    d_context = jnp.einsum('te,de->td', d_h, w_attn_out, preferred_element_type=jnp.float32).astype(jnp.bfloat16)
    d_qkv = attend_back(qkv_rot, d_context, cos_t, sin_t, num_seqs)
    d_w_qkv = jnp.einsum('td,te->de', normed1, d_qkv, preferred_element_type=jnp.float32)
    d_x, d_norm1_gain = input_grad(d_qkv, w_qkv, x_rows, norm1_gain, d_h)
    small = jnp.concatenate([d_w_router, d_norm1_gain.T, d_norm2_gain[:, None]], axis=1)
    return d_x, d_qkv, (d_w_qkv, d_w_attn_out, small)


def solution(mesh):
    ep_size, dp_size = mesh.shape['ep'], mesh.shape['dp']
    num_dev = ep_size * dp_size
    tok_spec = P(('dp', 'ep'), None, None)
    rep_spec = P()
    exp_spec = P('ep', None, None)

    def swap(value, distance):
        return lax.ppermute(value, ('dp', 'ep'), [(r, r ^ distance) for r in range(num_dev)])

    def spread_routes(value):
        return [value] + [swap(value, distance) for distance in range(1, num_dev)]

    def local_step(x_tokens, dy_tokens, route_idx, norm1_gain, norm2_gain, w_qkv, w_attn_out, w_router, w_gate, w_up, w_down):
        num_seqs, seq_len, model_width = x_tokens.shape
        num_tokens = num_seqs * seq_len
        top_k = route_idx.shape[-1]
        local_experts = w_gate.shape[0]
        num_experts = local_experts * ep_size
        capacity = capacity_rows(num_tokens, top_k, num_experts)
        x_rows = x_tokens.reshape(num_tokens, model_width)
        dy_rows = dy_tokens.reshape(num_tokens, model_width)
        idx_rows = route_idx.reshape(num_tokens, top_k)
        ep_rank = lax.axis_index('ep')
        me = lax.axis_index('dp') * ep_size + ep_rank
        first_expert = ep_rank * local_experts

        dy_all = lax.all_gather(dy_rows, ('dp', 'ep'), axis=0, tiled=True)
        idx_parts = spread_routes(idx_rows.T)
        dy_pair = swap(dy_rows, 1)
        routes = slot_positions(jnp.stack(idx_parts), first_expert, local_experts, capacity)

        cos_t, sin_t = rope_tables(seq_len)
        normed1, qkv_rot = qkv_project(x_rows, norm1_gain, w_qkv, cos_t, sin_t)
        qkv_rot, routes = lax.optimization_barrier((qkv_rot, routes))
        context = attend(qkv_rot, num_seqs)
        h_rows = (x_rows.astype(jnp.float32) + jnp.dot(context, w_attn_out, preferred_element_type=jnp.float32)).astype(jnp.bfloat16)
        normed2 = rms_norm(h_rows, norm2_gain)
        x_pair = swap(normed2, 1)
        logits = jnp.dot(normed2, w_router, preferred_element_type=jnp.float32)
        probs_all, hits, picked_sum = gate_forward(logits, idx_rows, num_experts)
        gates = probs_all * hits / picked_sum
        gate_t = jnp.sum(jnp.where(choice_mask(idx_rows, num_experts), gates[:, None, :], 0.0), axis=2).T
        x_all = lax.all_gather(normed2, ('dp', 'ep'), axis=0, tiled=True)
        gate_parts = spread_routes(gate_t)
        gate_near, gate_x, gate_far = (expand_routes(jnp.stack(idx_parts[lo:hi]), jnp.stack(gate_parts[lo:hi]), first_expert, local_experts)
                                       for lo, hi in ((0, 2), (2, ep_size), (ep_size, num_dev)))

        gather = functools.partial(gather_slots, me[None], routes, own_dev=ep_size, capacity=capacity)
        rows_of = lambda a: a.reshape(local_experts, -1, a.shape[-1])
        slots_of = lambda a, n: a.reshape(local_experts, n, capacity, a.shape[-1])
        combine = functools.partial(combine_slots, ep_rank[None], routes, total_dev=ep_size)
        weights = (w_gate, w_up, w_down)
        tile = 2 * capacity
        arrays = gather(0, 1, gate_near[:1], normed2, dy_rows, None, scaled=False, from_all=False)
        s_arr, dy_arr, g_arr = gather(1, 1, gate_near[1:], x_pair, dy_pair, arrays, scaled=False, from_all=False)
        hidden, dag, dau, d_out, ds_near, dg_near = expert_pass(True, tile, 0, 1, rows_of(s_arr), rows_of(dy_arr), rows_of(g_arr), *weights, None)
        combined = combine(0, 2, d_slots=slots_of(ds_near, 2), d_gate_slots=slots_of(dg_near, 2), filled=None)
        s_arr, dy_arr, g_arr = gather(2, 2, gate_x, x_all, dy_all, (s_arr, slots_of(d_out, num_dev), g_arr), scaled=False, from_all=True)
        hidden, dag, dau, d_out, ds_x, dg_x = expert_pass(True, tile, 1, 1, rows_of(s_arr), rows_of(dy_arr), rows_of(g_arr), *weights, (hidden, dag, dau))
        d_tok, d_gate_t = combine(2, 2, d_slots=slots_of(ds_x, 2), d_gate_slots=slots_of(dg_x, 2), filled=combined)
        d_normed2_moe = lax.psum_scatter(d_tok, 'ep', scatter_dimension=0, tiled=True)
        d_gate_blk = lax.all_to_all(d_gate_t, 'ep', 0, 0, tiled=True)
        d_gate_dense = jnp.transpose(d_gate_blk, (1, 3, 0, 2)).reshape(num_tokens, num_experts)
        d_out, _ = lax.optimization_barrier((d_out, d_tok))
        s_arr, dy_arr = gather(4, 4, gate_far, x_all, dy_all, (s_arr, slots_of(d_out, num_dev)), scaled=True, from_all=True)
        s_all, d_out = rows_of(s_arr), rows_of(dy_arr)
        hidden, dag, dau = expert_pass(False, 2 * tile, 1, 1, s_all, d_out, None, *weights, (hidden, dag, dau))
        hidden, d_normed2_moe = lax.optimization_barrier((hidden, d_normed2_moe))
        d_w_down, = weight_grads(hidden, d_out)

        d_logits = gate_backward(probs_all, hits, picked_sum, d_gate_dense).astype(jnp.bfloat16)
        saved_state = (normed1, qkv_rot, context, h_rows, normed2, cos_t, sin_t, num_seqs)
        d_x, d_qkv, dense_grads = dense_backward(saved_state, x_rows, dy_rows, d_logits, d_normed2_moe, norm1_gain, norm2_gain, w_qkv, w_attn_out, w_router)
        d_w_qkv, d_w_attn_out, small = lax.psum(dense_grads, ('dp', 'ep'))
        s_all, dag, dau, _ = lax.optimization_barrier((s_all, dag, dau, d_qkv))
        d_w_gate, d_w_up = weight_grads(s_all, dag, dau)
        return (d_x.reshape(x_tokens.shape), small[:, num_experts], small[:, num_experts + 1], d_w_qkv, d_w_attn_out, small[:, :num_experts],
                d_w_gate, d_w_up, d_w_down)

    return jax.shard_map(local_step, mesh=mesh,
                         in_specs=(tok_spec, tok_spec, tok_spec, rep_spec, rep_spec, rep_spec, rep_spec, rep_spec, exp_spec, exp_spec, exp_spec),
                         out_specs=(tok_spec, rep_spec, rep_spec, rep_spec, rep_spec, rep_spec, exp_spec, exp_spec, exp_spec),
                         check_vma=False)
```

```python
import functools

import jax
import jax.numpy as jnp
from jax import lax
from jax.experimental import pallas as pl
from jax.experimental.pallas import tpu as pltpu
from jax.sharding import PartitionSpec as P

EPS = 1e-6
HEAD_DIM = 128
ROPE_BASE = 10000.0
TOK_BLOCK = 256
WIN = 64
ALIGN = 16
GROUP = 4
VMEM_MAX = 64 * 1024 * 1024 - 65536


def capacity_rows(num_tokens, top_k, num_experts):
    return 8 * ((5 * num_tokens * top_k + 32 * num_experts - 1) // (32 * num_experts))


def dot_nn(left, right):
    return jnp.dot(left, right, preferred_element_type=jnp.float32)


def dot_nt(left, right):
    return lax.dot_general(left, right, (((1,), (1,)), ((), ())), preferred_element_type=jnp.float32)


def dot_tn(left, right):
    return lax.dot_general(left, right, (((0,), (0,)), ((), ())), preferred_element_type=jnp.float32)


def rope_tables(seq_len):
    half_dim = HEAD_DIM // 2
    inv_freq = ROPE_BASE ** (-jnp.arange(half_dim, dtype=jnp.float32) / half_dim)
    angles = jnp.arange(seq_len, dtype=jnp.float32)[:, None] * inv_freq[None, :]
    cos_b, sin_b = jnp.cos(angles), jnp.sin(angles)
    return jnp.concatenate([cos_b, cos_b], axis=1), jnp.concatenate([-sin_b, sin_b], axis=1)


def unit_rms(rows_f32):
    return lax.rsqrt(jnp.mean(rows_f32 * rows_f32, axis=-1, keepdims=True) + EPS)


def join_heads(ref):
    return jnp.concatenate([ref[h] for h in range(ref.shape[0])], axis=1)


def qkv_kernel(x_ref, gain_ref, w_ref, cos_ref, sin_ref, normed_t_ref, qkv_ref, *, rotated, chunk):
    x_f32 = x_ref[...].astype(jnp.float32)
    normed = (x_f32 * unit_rms(x_f32) * gain_ref[...]).astype(jnp.bfloat16)
    normed_t_ref[...] = jnp.transpose(normed)
    for c in range(0, w_ref.shape[1], chunk):
        acc = dot_nn(normed, w_ref[:, c:c + chunk])
        for h in range(0, chunk, HEAD_DIM):
            head = acc[:, h:h + HEAD_DIM]
            if c + h < rotated:
                head = head * cos_ref[...] + pltpu.roll(head, HEAD_DIM // 2, 1) * sin_ref[...]
            qkv_ref[(c + h) // HEAD_DIM] = head.astype(jnp.bfloat16)


def qkv_project(x_rows, gain_row, w_qkv, cos_t, sin_t):
    num_tokens, width = x_rows.shape
    seq_len = cos_t.shape[0]
    tile = min(512, seq_len)
    per_seq = seq_len // tile
    heads = 3 * width // HEAD_DIM
    row_spec = pl.BlockSpec((tile, width), lambda r: (r, 0))
    table_spec = pl.BlockSpec((tile, HEAD_DIM), lambda r: (lax.rem(r, per_seq), 0))
    return pl.pallas_call(
        functools.partial(qkv_kernel, rotated=2 * width, chunk=256),
        out_shape=[jax.ShapeDtypeStruct((width, num_tokens), jnp.bfloat16), jax.ShapeDtypeStruct((heads, num_tokens, HEAD_DIM), jnp.bfloat16)],
        grid=(num_tokens // tile,),
        in_specs=[row_spec, pl.BlockSpec((1, width), lambda r: (0, 0)), pl.BlockSpec((width, 3 * width), lambda r: (0, 0)), table_spec, table_spec],
        out_specs=[pl.BlockSpec((width, tile), lambda r: (0, r)), pl.BlockSpec((heads, tile, HEAD_DIM), lambda r: (0, r, 0))],
        compiler_params=pltpu.CompilerParams(vmem_limit_bytes=VMEM_MAX, dimension_semantics=('arbitrary',)),
        cost_estimate=pl.CostEstimate(flops=6 * num_tokens * width * width, bytes_accessed=2 * width * (5 * num_tokens + 3 * width), transcendentals=num_tokens),
        name='qkv_project',
    )(x_rows, gain_row, w_qkv, cos_t, sin_t)


def attend_kernel(q_all, k_all, v_all, ctx_all, *, block):
    count, seq_len, _ = q_all.shape
    diag = lax.broadcasted_iota(jnp.int32, (block, block), 0) >= lax.broadcasted_iota(jnp.int32, (block, block), 1)
    for head in range(count):
        q_ref, k_ref, v_ref, ctx_ref = (ref.at[head] for ref in (q_all, k_all, v_all, ctx_all))
        for start in range(0, seq_len, block):
            stop = start + block
            scores = dot_nt(q_ref[start:stop, :], k_ref[:stop, :]) * HEAD_DIM ** -0.5
            last = jnp.where(diag, scores[:, start:], -1e30)
            scores = last if start == 0 else jnp.concatenate([scores[:, :start], last], axis=1)
            raised = jnp.exp(scores - jnp.max(scores, axis=1, keepdims=True))
            probs = (raised * (1.0 / jnp.sum(raised, axis=1, keepdims=True))).astype(jnp.bfloat16)
            ctx_ref[start:stop, :] = dot_nn(probs, v_ref[:stop, :]).astype(jnp.bfloat16)


def head_spec(seq_len, offset, heads=1):
    return pl.BlockSpec((heads, seq_len, HEAD_DIM), lambda s, h: (h + offset // heads, s, 0))


def attend(qkv_rot, num_seqs):
    heads, num_tokens = qkv_rot.shape[0] // 3, qkv_rot.shape[1]
    seq_len, width = num_tokens // num_seqs, heads * HEAD_DIM
    return pl.pallas_call(
        functools.partial(attend_kernel, block=min(256, seq_len)),
        out_shape=jax.ShapeDtypeStruct((heads, num_tokens, HEAD_DIM), jnp.bfloat16),
        grid=(num_seqs, heads // 2),
        in_specs=[head_spec(seq_len, 0, 2), head_spec(seq_len, heads, 2), head_spec(seq_len, 2 * heads, 2)],
        out_specs=head_spec(seq_len, 0, 2),
        compiler_params=pltpu.CompilerParams(vmem_limit_bytes=VMEM_MAX, dimension_semantics=('arbitrary', 'arbitrary')),
        cost_estimate=pl.CostEstimate(flops=4 * num_tokens * seq_len * width, bytes_accessed=8 * num_tokens * width, transcendentals=num_tokens * seq_len * heads),
        name='attend',
    )(qkv_rot, qkv_rot, qkv_rot)


def attend_back_kernel(q_ref, k_ref, v_ref, dctx_ref, cos_ref, sin_ref, out_ref, d_key, d_val, *, block):
    seq_len = q_ref.shape[1]
    scale = HEAD_DIM ** -0.5
    causal = lax.broadcasted_iota(jnp.int32, (block, block), 0) <= lax.broadcasted_iota(jnp.int32, (block, block), 1)

    def unrotate(grad, cos, sin):
        grad = grad.astype(jnp.bfloat16).astype(jnp.float32)
        return (grad * cos + pltpu.roll(grad * sin, HEAD_DIM // 2, 1)).astype(jnp.bfloat16)

    key_t = jnp.transpose(k_ref[0])
    for start in range(0, seq_len, block):
        stop = start + block
        query, d_ctx = q_ref[0, start:stop, :], dctx_ref[0, start:stop, :]
        scores = dot_nt(k_ref[0, :stop, :], query) * scale
        last = jnp.where(causal, scores[start:, :], -1e30)
        scores = last if start == 0 else jnp.concatenate([scores[:start, :], last], axis=0)
        raised = jnp.exp(scores - jnp.max(scores, axis=0, keepdims=True))
        probs = raised * (1.0 / jnp.sum(raised, axis=0, keepdims=True))
        d_probs = dot_nt(v_ref[0, :stop, :], d_ctx).astype(jnp.bfloat16).astype(jnp.float32)
        mean_d = jnp.sum(d_probs * probs, axis=0, keepdims=True)
        d_scores = (probs * (d_probs - mean_d) * scale).astype(jnp.bfloat16)
        d_v = dot_nn(probs.astype(jnp.bfloat16), d_ctx)
        d_k = dot_nn(d_scores, query)
        if start == 0:
            d_val[:stop, :] = d_v
            d_key[:stop, :] = d_k
        else:
            d_val[:start, :] += d_v[:start]
            d_key[:start, :] += d_k[:start]
            d_val[start:stop, :] = d_v[start:]
            d_key[start:stop, :] = d_k[start:]
        d_q = jnp.transpose(dot_nn(key_t[:, :stop], d_scores))
        out_ref[0, 0, start:stop, :] = unrotate(d_q, cos_ref[start:stop, :], sin_ref[start:stop, :])
    out_ref[1, 0] = unrotate(d_key[...], cos_ref[...], sin_ref[...])
    out_ref[2, 0] = d_val[...].astype(jnp.bfloat16)


def attend_back(qkv_rot, d_context, cos_t, sin_t, num_seqs):
    heads, num_tokens, _ = d_context.shape
    seq_len, width = num_tokens // num_seqs, heads * HEAD_DIM
    table_spec = pl.BlockSpec((seq_len, HEAD_DIM), lambda s, h: (0, 0))
    return pl.pallas_call(
        functools.partial(attend_back_kernel, block=min(256, seq_len)),
        out_shape=jax.ShapeDtypeStruct((3, heads, num_tokens, HEAD_DIM), jnp.bfloat16),
        grid=(num_seqs, heads),
        in_specs=[head_spec(seq_len, 0), head_spec(seq_len, heads), head_spec(seq_len, 2 * heads), head_spec(seq_len, 0), table_spec, table_spec],
        out_specs=pl.BlockSpec((3, 1, seq_len, HEAD_DIM), lambda s, h: (0, h, s, 0)),
        scratch_shapes=[pltpu.VMEM((seq_len, HEAD_DIM), jnp.float32), pltpu.VMEM((seq_len, HEAD_DIM), jnp.float32)],
        compiler_params=pltpu.CompilerParams(vmem_limit_bytes=VMEM_MAX, dimension_semantics=('arbitrary', 'arbitrary')),
        cost_estimate=pl.CostEstimate(flops=10 * num_tokens * seq_len * width, bytes_accessed=14 * num_tokens * width, transcendentals=num_tokens * seq_len * heads),
        name='attend_back',
    )(qkv_rot, qkv_rot, qkv_rot, d_context, cos_t, sin_t).reshape(3 * heads, num_tokens, HEAD_DIM)


def choice_hits(idx_ref, shape):
    lanes = lax.broadcasted_iota(jnp.int32, shape, 1)
    hits = jnp.zeros(shape, jnp.float32)
    for k in range(idx_ref.shape[1]):
        hits += jnp.where(idx_ref[:, k:k + 1] == lanes, 1.0, 0.0)
    return hits


def router_kernel(ctx_ref, w_ref, x_ref, gain_ref, router_ref, idx_ref, h_ref, normed_ref, probs_ref, gate_ref, *, ranks, local_experts):
    hidden = (x_ref[...].astype(jnp.float32) + dot_nn(join_heads(ctx_ref), w_ref[...])).astype(jnp.bfloat16)
    h_ref[...] = hidden
    h_f32 = hidden.astype(jnp.float32)
    normed = (h_f32 * unit_rms(h_f32) * gain_ref[...]).astype(jnp.bfloat16)
    normed_ref[...] = normed
    logits = dot_nn(normed, router_ref[...])
    lanes = lax.broadcasted_iota(jnp.int32, logits.shape, 1)
    logits = jnp.where(lanes < ranks * local_experts, logits, -jnp.inf)
    raised = jnp.exp(logits - jnp.max(logits, axis=1, keepdims=True))
    probs = raised / jnp.sum(raised, axis=1, keepdims=True)
    probs_ref[...] = probs
    picked = probs * choice_hits(idx_ref, probs.shape)
    gates = picked / jnp.sum(picked, axis=1, keepdims=True)
    for blk in range(gates.shape[0] // TOK_BLOCK):
        gate_t = jnp.transpose(gates[blk * TOK_BLOCK:(blk + 1) * TOK_BLOCK, :])
        for rank in range(ranks):
            gate_ref[rank, blk] = gate_t[rank * local_experts:(rank + 1) * local_experts, :]


def route_tokens(context, w_attn_out, x_rows, gain_row, router_pad, idx_rows, ranks, local_experts):
    heads, num_tokens, _ = context.shape
    width, lanes = x_rows.shape[1], router_pad.shape[1]
    tile = min(512, num_tokens)
    row_spec = pl.BlockSpec((tile, width), lambda r: (r, 0))
    whole = lambda shape: pl.BlockSpec(shape, lambda r: (0,) * len(shape))
    return pl.pallas_call(
        functools.partial(router_kernel, ranks=ranks, local_experts=local_experts),
        out_shape=[jax.ShapeDtypeStruct((num_tokens, width), jnp.bfloat16), jax.ShapeDtypeStruct((num_tokens, width), jnp.bfloat16),
                   jax.ShapeDtypeStruct((num_tokens, lanes), jnp.float32),
                   jax.ShapeDtypeStruct((ranks, num_tokens // TOK_BLOCK, local_experts, TOK_BLOCK), jnp.float32)],
        grid=(num_tokens // tile,),
        in_specs=[pl.BlockSpec((heads, tile, HEAD_DIM), lambda r: (0, r, 0)), whole((width, width)), row_spec, whole((1, width)), whole((width, lanes)),
                  pl.BlockSpec((tile, idx_rows.shape[1]), lambda r: (r, 0))],
        out_specs=[row_spec, row_spec, pl.BlockSpec((tile, lanes), lambda r: (r, 0)),
                   pl.BlockSpec((ranks, tile // TOK_BLOCK, local_experts, TOK_BLOCK), lambda r: (0, r, 0, 0))],
        compiler_params=pltpu.CompilerParams(vmem_limit_bytes=VMEM_MAX, dimension_semantics=('arbitrary',)),
        cost_estimate=pl.CostEstimate(flops=2 * num_tokens * width * (width + lanes), bytes_accessed=2 * width * (4 * num_tokens + width), transcendentals=num_tokens * lanes),
        name='route_tokens',
    )(context, w_attn_out, x_rows, gain_row, router_pad, idx_rows)


def attn_out_grad_kernel(moe_ref, probs_ref, idx_ref, dgate_ref, h_ref, normed_ref, ctx_ref, dy_ref, gain_ref, router_ref, w_ref,
                         dh_ref, dctx_ref, drouter_ref, dgain_ref, dw_ref, *, ranks, local_experts):
    @pl.when(pl.program_id(0) == 0)
    def _():
        drouter_ref[...] = jnp.zeros_like(drouter_ref)
        dgain_ref[...] = jnp.zeros_like(dgain_ref)
        dw_ref[...] = jnp.zeros_like(dw_ref)

    probs = probs_ref[...]
    hits = choice_hits(idx_ref, probs.shape)
    picked_sum = jnp.sum(probs * hits, axis=1, keepdims=True)
    gates = probs * hits / picked_sum
    blank = jnp.zeros((probs.shape[1] - ranks * local_experts, TOK_BLOCK), jnp.float32)
    d_gates = jnp.concatenate([jnp.transpose(jnp.concatenate([dgate_ref[rank, blk] for rank in range(ranks)] + [blank], axis=0))
                               for blk in range(dgate_ref.shape[1])], axis=0)
    d_probs = hits * (d_gates - jnp.sum(d_gates * gates, axis=1, keepdims=True)) / picked_sum
    d_logits = (probs * (d_probs - jnp.sum(d_probs * probs, axis=1, keepdims=True))).astype(jnp.bfloat16)
    drouter_ref[...] += dot_tn(normed_ref[...], d_logits)
    d_normed = moe_ref[...] + dot_nt(d_logits, router_ref[...])
    h_f32 = h_ref[...].astype(jnp.float32)
    inv_rms = unit_rms(h_f32)
    dgain_ref[...] += jnp.sum(d_normed * h_f32 * inv_rms, axis=0, keepdims=True)
    d_scaled = d_normed * gain_ref[...]
    d_part = inv_rms * d_scaled - h_f32 * (inv_rms * inv_rms * inv_rms) * jnp.mean(d_scaled * h_f32, axis=-1, keepdims=True)
    d_hidden = (dy_ref[...].astype(jnp.float32) + d_part).astype(jnp.bfloat16)
    dh_ref[...] = d_hidden
    d_ctx = dot_nt(d_hidden, w_ref[...]).astype(jnp.bfloat16)
    for head in range(dctx_ref.shape[0]):
        dctx_ref[head] = d_ctx[:, head * HEAD_DIM:(head + 1) * HEAD_DIM]
    dw_ref[...] += dot_tn(join_heads(ctx_ref), d_hidden)


def attn_out_grad(d_normed_moe, probs, idx_rows, d_gate_blk, h_rows, normed, context, dy_rows, gain_row, router_pad, w_attn_out):
    heads, num_tokens, _ = context.shape
    width, lanes = h_rows.shape[1], router_pad.shape[1]
    ranks, _, local_experts, _ = d_gate_blk.shape
    tile = min(512, num_tokens)
    row_spec = pl.BlockSpec((tile, width), lambda r: (r, 0))
    head_rows = pl.BlockSpec((heads, tile, HEAD_DIM), lambda r: (0, r, 0))
    whole = lambda shape: pl.BlockSpec(shape, lambda r: (0,) * len(shape))
    return pl.pallas_call(
        functools.partial(attn_out_grad_kernel, ranks=ranks, local_experts=local_experts),
        out_shape=[jax.ShapeDtypeStruct((num_tokens, width), jnp.bfloat16), jax.ShapeDtypeStruct(context.shape, jnp.bfloat16),
                   jax.ShapeDtypeStruct((width, lanes), jnp.float32), jax.ShapeDtypeStruct((1, width), jnp.float32),
                   jax.ShapeDtypeStruct((width, width), jnp.float32)],
        grid=(num_tokens // tile,),
        in_specs=[row_spec, pl.BlockSpec((tile, lanes), lambda r: (r, 0)), pl.BlockSpec((tile, idx_rows.shape[1]), lambda r: (r, 0)),
                  pl.BlockSpec((ranks, tile // TOK_BLOCK, local_experts, TOK_BLOCK), lambda r: (0, r, 0, 0)), row_spec, row_spec, head_rows, row_spec,
                  whole((1, width)), whole((width, lanes)), whole((width, width))],
        out_specs=[row_spec, head_rows, whole((width, lanes)), whole((1, width)), whole((width, width))],
        compiler_params=pltpu.CompilerParams(vmem_limit_bytes=VMEM_MAX, dimension_semantics=('arbitrary',)),
        cost_estimate=pl.CostEstimate(flops=4 * num_tokens * width * (width + lanes), bytes_accessed=2 * width * (8 * num_tokens + 3 * width), transcendentals=num_tokens),
        name='attn_out_grad',
    )(d_normed_moe, probs, idx_rows, d_gate_blk, h_rows, normed, context, dy_rows, gain_row, router_pad, w_attn_out)


def qkv_grad_kernel(normed_t_ref, dqkv_ref, dw_ref):
    dw_ref[...] = dot_nn(normed_t_ref[...], join_heads(dqkv_ref))


def qkv_grad(normed_t, d_qkv):
    width, num_tokens = normed_t.shape
    heads = d_qkv.shape[0]
    group = 2 if heads % 4 else 4
    return pl.pallas_call(
        qkv_grad_kernel,
        out_shape=jax.ShapeDtypeStruct((width, heads * HEAD_DIM), jnp.float32),
        grid=(heads // group,),
        in_specs=[pl.BlockSpec((width, num_tokens), lambda c: (0, 0)), pl.BlockSpec((group, num_tokens, HEAD_DIM), lambda c: (c, 0, 0))],
        out_specs=pl.BlockSpec((width, group * HEAD_DIM), lambda c: (0, c)),
        compiler_params=pltpu.CompilerParams(vmem_limit_bytes=VMEM_MAX, dimension_semantics=('arbitrary',)),
        cost_estimate=pl.CostEstimate(flops=6 * num_tokens * width * width, bytes_accessed=2 * width * (4 * num_tokens + 6 * width), transcendentals=0),
        name='qkv_grad',
    )(normed_t, d_qkv)


def input_grad_kernel(dqkv_ref, w_ref, x_ref, gain_ref, dh_ref, dx_ref, dgain_ref):
    d_out = dot_nt(join_heads(dqkv_ref), w_ref[...])
    x_f32 = x_ref[...].astype(jnp.float32)
    inv_rms = unit_rms(x_f32)
    part = jnp.sum(d_out * x_f32 * inv_rms, axis=0, keepdims=True)

    @pl.when(pl.program_id(0) == 0)
    def _():
        dgain_ref[...] = jnp.zeros_like(dgain_ref)

    dgain_ref[...] += part
    d_scaled = d_out * gain_ref[...]
    d_x = inv_rms * d_scaled - x_f32 * (inv_rms * inv_rms * inv_rms) * jnp.mean(d_scaled * x_f32, axis=-1, keepdims=True)
    dx_ref[...] = (dh_ref[...].astype(jnp.float32) + d_x).astype(jnp.bfloat16)


def input_grad(d_qkv, w_qkv, x_rows, gain_row, d_h):
    num_tokens, width = x_rows.shape
    tile = min(512, num_tokens)
    row_spec = pl.BlockSpec((tile, width), lambda r: (r, 0))
    gain_spec = pl.BlockSpec((1, width), lambda r: (0, 0))
    return pl.pallas_call(
        input_grad_kernel,
        out_shape=[jax.ShapeDtypeStruct((num_tokens, width), jnp.bfloat16), jax.ShapeDtypeStruct((1, width), jnp.float32)],
        grid=(num_tokens // tile,),
        in_specs=[pl.BlockSpec((d_qkv.shape[0], tile, HEAD_DIM), lambda r: (0, r, 0)), pl.BlockSpec((width, 3 * width), lambda r: (0, 0)), row_spec, gain_spec, row_spec],
        out_specs=[row_spec, gain_spec],
        compiler_params=pltpu.CompilerParams(vmem_limit_bytes=VMEM_MAX, dimension_semantics=('arbitrary',)),
        cost_estimate=pl.CostEstimate(flops=6 * num_tokens * width * width, bytes_accessed=2 * width * (6 * num_tokens + 3 * width), transcendentals=num_tokens),
        name='input_grad',
    )(d_qkv, w_qkv, x_rows, gain_row, d_h)


def slot_positions(idx_t, first_expert, local_experts, capacity):
    num_dev, _, num_tokens = idx_t.shape
    experts = first_expert + jnp.arange(local_experts, dtype=jnp.int32)
    hits = jnp.sum((idx_t[:, None, :, :] == experts[None, :, None, None]).astype(jnp.float32), axis=2)
    blocks = num_tokens // TOK_BLOCK
    hit_blk = hits.reshape(num_dev, local_experts, blocks, TOK_BLOCK)
    upto = (jnp.arange(TOK_BLOCK)[:, None] <= jnp.arange(TOK_BLOCK)[None, :]).astype(jnp.bfloat16)
    within = jnp.einsum('debt,tu->debu', hit_blk.astype(jnp.bfloat16), upto, preferred_element_type=jnp.float32)
    totals = jnp.sum(hit_blk, axis=-1)
    strict = (jnp.arange(blocks)[:, None] < jnp.arange(blocks)[None, :])
    before = jnp.sum(jnp.where(strict[None, None], totals[:, :, :, None], 0.0), axis=2)
    position = (within + before[..., None] - 1.0).astype(jnp.int32)
    slot_of = jnp.where((hit_blk > 0) & (position < capacity), position, -1)
    begin = jnp.minimum(before.astype(jnp.int32), capacity)
    end = jnp.minimum((before + totals).astype(jnp.int32), capacity)
    win_start = jnp.minimum(begin // ALIGN * ALIGN, capacity - WIN)
    win_count = jnp.maximum((end - win_start + WIN - 1) // WIN, 1)
    filled = jnp.max(end, axis=2)
    most_group = jnp.max(win_count.reshape(num_dev, local_experts // GROUP, GROUP * blocks), axis=2)
    most_block = jnp.max(win_count, axis=1)
    return jnp.transpose(slot_of, (0, 2, 1, 3)), begin.reshape(-1), win_count.reshape(-1), most_group.reshape(-1), most_block.reshape(-1), filled.reshape(-1)


def window_start(begin, capacity):
    return jnp.minimum(lax.div(begin, ALIGN) * ALIGN, capacity - WIN)


def gather_kernel(base_ref, begin_ref, count_ref, most_ref, fill_ref, x_ref, dy_ref, slot_ref, gate_ref, *rest, blocks, capacity, group, scaled, dev_from):
    s_ref, dyr_ref = rest[-2:] if scaled else rest[-3:-1]
    g_ref = None if scaled else rest[-1]
    dev, part = pl.program_id(0) + dev_from, pl.program_id(1)
    experts = group * pl.num_programs(1)
    overflow = most_ref[dev * pl.num_programs(1) + part] > 1

    @pl.when(overflow)
    def _():
        s_ref[...] = jnp.zeros_like(s_ref)
        dyr_ref[...] = jnp.zeros_like(dyr_ref)

    if g_ref is not None:
        g_ref[...] = jnp.zeros_like(g_ref)
    cleared = max(capacity - 128, 0) // ALIGN * ALIGN
    for ref in (s_ref, dyr_ref):
        ref[:, 0, cleared:, :] = jnp.zeros((group, capacity - cleared, ref.shape[-1]), jnp.bfloat16)
    row_iota = lax.broadcasted_iota(jnp.int32, (WIN, TOK_BLOCK), 0)
    line_iota = lax.broadcasted_iota(jnp.int32, (WIN, x_ref.shape[1]), 0)

    def at(i, blk):
        return (dev * experts + part * group + i) * blocks + blk

    def window(i, blk, first, floor=None):
        slot_row = slot_ref[0, blk, pl.ds(part * group + i, 1), :]
        hit = slot_row == row_iota + first
        if floor is not None:
            hit = hit & (slot_row >= floor)
        gate_row = gate_ref[0, blk, pl.ds(part * group + i, 1), :]
        gate_col = jnp.sum(jnp.where(hit, gate_row, 0.0), axis=1, keepdims=True)
        return jnp.where(hit, 1.0, 0.0).astype(jnp.bfloat16), gate_col

    def deposit(i, first, s_rows, dy_rows, gate_col, begin=None):
        rows = pl.ds(pl.multiple_of(first, ALIGN), WIN)
        s_rows = s_rows.astype(jnp.bfloat16)
        dy_rows = (dy_rows * gate_col if scaled else dy_rows).astype(jnp.bfloat16)
        if begin is None:
            s_ref[i, 0, rows, :] += s_rows
            dyr_ref[i, 0, rows, :] += dy_rows
        else:
            earlier = line_iota < begin - first
            s_ref[i, 0, rows, :] = jnp.where(earlier, s_ref[i, 0, rows, :], s_rows)
            dyr_ref[i, 0, rows, :] = jnp.where(earlier, dyr_ref[i, 0, rows, :], dy_rows)
        if not scaled:
            g_ref[i, 0, rows, :] += gate_col

    for blk in range(blocks):
        tokens = slice(blk * TOK_BLOCK, (blk + 1) * TOK_BLOCK)
        begins = [begin_ref[at(i, blk)] for i in range(group)]
        firsts = [window_start(begin, capacity) for begin in begins]
        parts = [window(i, blk, firsts[i]) for i in range(group)]
        pick = jnp.concatenate([p[0] for p in parts], axis=0)
        s_all = jnp.dot(pick, x_ref[tokens, :], preferred_element_type=jnp.float32)
        dy_all = jnp.dot(pick, dy_ref[tokens, :], preferred_element_type=jnp.float32)
        for i in range(group):
            rows = slice(i * WIN, (i + 1) * WIN)
            deposit(i, firsts[i], s_all[rows], dy_all[rows], parts[i][1], begins[i])

    for i in range(group):
        def blank(step, carry):
            rows = pl.ds(pl.multiple_of(step * ALIGN, ALIGN), ALIGN)
            s_ref[i, 0, rows, :] = jnp.zeros((ALIGN, s_ref.shape[-1]), jnp.bfloat16)
            dyr_ref[i, 0, rows, :] = jnp.zeros((ALIGN, s_ref.shape[-1]), jnp.bfloat16)
            return carry

        lax.fori_loop(lax.div(fill_ref[dev * experts + part * group + i] + ALIGN - 1, ALIGN), cleared // ALIGN, blank, 0)

    @pl.when(overflow)
    def _():
        for i in range(group):
            def per_block(blk, carry):
                def extra(w, inner):
                    floor = window_start(begin_ref[at(i, blk)], capacity) + w * WIN
                    first = jnp.minimum(floor, capacity - WIN)
                    pick, gate_col = window(i, blk, first, floor)
                    tokens = pl.ds(pl.multiple_of(blk * TOK_BLOCK, TOK_BLOCK), TOK_BLOCK)
                    s_rows = jnp.dot(pick, x_ref[tokens, :], preferred_element_type=jnp.float32)
                    dy_rows = jnp.dot(pick, dy_ref[tokens, :], preferred_element_type=jnp.float32)
                    deposit(i, first, s_rows, dy_rows, gate_col)
                    return inner

                return lax.fori_loop(1, count_ref[at(i, blk)], extra, carry)

            lax.fori_loop(0, blocks, per_block, 0)


def gather_slots(base_dev, routes, dev_from, num_dev, gate_of, x_table, dy_table, filled, own_dev, capacity, scaled, from_all):
    slot_of, begin, win_count, most, _, fill = routes
    total_dev, blocks, experts, _ = slot_of.shape
    width = x_table.shape[1]
    num_tokens = blocks * TOK_BLOCK
    group = GROUP

    def table_map(d, p, base_ref, *_):
        return (lax.bitwise_xor(d + dev_from, base_ref[0]) if from_all else 0, 0)

    def slot_map(d, p, *_):
        return (d + dev_from, 0, 0, 0)

    def gate_map(d, p, *_):
        return (d, 0, 0, 0)

    def out_map(d, p, *_):
        return (p, d + dev_from, 0, 0)

    rows_shape = jax.ShapeDtypeStruct((experts, total_dev, capacity, width), jnp.bfloat16)
    row_spec = pl.BlockSpec((group, 1, capacity, width), out_map)
    out_shape, out_specs = [rows_shape, rows_shape], [row_spec, row_spec]
    if not scaled:
        out_shape.append(jax.ShapeDtypeStruct((experts, own_dev, capacity, 1), jnp.float32))
        out_specs.append(pl.BlockSpec((group, 1, capacity, 1), out_map))
    held = () if filled is None else tuple(filled)
    route_block = (1, blocks, experts, TOK_BLOCK)
    return pl.pallas_call(
        functools.partial(gather_kernel, blocks=blocks, capacity=capacity, group=group, scaled=scaled, dev_from=dev_from),
        out_shape=out_shape,
        grid_spec=pltpu.PrefetchScalarGridSpec(
            num_scalar_prefetch=5, grid=(num_dev, experts // group),
            in_specs=[pl.BlockSpec((num_tokens, width), table_map), pl.BlockSpec((num_tokens, width), table_map),
                      pl.BlockSpec(route_block, slot_map), pl.BlockSpec(route_block, gate_map)]
                     + [pl.BlockSpec(memory_space=pl.ANY)] * len(held),
            out_specs=out_specs),
        input_output_aliases={9 + i: i for i in range(len(held))},
        compiler_params=pltpu.CompilerParams(vmem_limit_bytes=VMEM_MAX, dimension_semantics=('arbitrary', 'arbitrary')),
        cost_estimate=pl.CostEstimate(flops=4 * num_dev * blocks * experts * WIN * TOK_BLOCK * width,
                                      bytes_accessed=4 * num_dev * (num_tokens + experts * capacity) * width, transcendentals=0),
        name='gather_slots',
    )(base_dev, begin, win_count, most, fill, x_table, dy_table, slot_of, gate_of, *held)


def expert_kernel(*refs, own, chunk, held):
    if own:
        s_ref, dy_ref, g_ref, wg_ref, wu_ref, wd_ref = refs[:6]
        hid_ref, dag_ref, dau_ref, do_ref, ds_ref, dgate_ref = refs[6 + held:]
        do_ref[0] = (dy_ref[0].astype(jnp.float32) * g_ref[0]).astype(jnp.bfloat16)
    else:
        s_ref, do_ref, wg_ref, wu_ref, wd_ref = refs[:5]
        hid_ref, dag_ref, dau_ref = refs[5 + held:]
    width = s_ref.shape[-1]
    for c in range(0, width, chunk):
        cols = slice(c, c + chunk)
        act_gate = dot_nn(s_ref[0], wg_ref[0, :, cols])
        act_up = dot_nn(s_ref[0], wu_ref[0, :, cols])
        d_hidden = dot_nt(do_ref[0], wd_ref[0, cols, :])
        sig = jax.nn.sigmoid(act_gate)
        silu = act_gate * sig
        hid_ref[0, :, cols] = (silu * act_up).astype(jnp.bfloat16)
        dau_ref[0, :, cols] = (d_hidden * silu).astype(jnp.bfloat16)
        dag_ref[0, :, cols] = (d_hidden * act_up * (sig + silu * (1.0 - sig))).astype(jnp.bfloat16)
    if own:
        d_gate = None
        for c in range(0, width, chunk):
            cols = slice(c, c + chunk)
            out = dot_nn(hid_ref[0], wd_ref[0, :, cols]).astype(jnp.bfloat16).astype(jnp.float32)
            part = jnp.sum(out * dy_ref[0, :, cols].astype(jnp.float32), axis=1, keepdims=True)
            d_gate = part if d_gate is None else d_gate + part
            ds_ref[0, :, cols] = (dot_nt(dag_ref[0], wg_ref[0, cols, :]) + dot_nt(dau_ref[0], wu_ref[0, cols, :])).astype(jnp.bfloat16)
        dgate_ref[0] = d_gate


def expert_pass(own, tile, first_tile, num_tiles, s_rows, dy_rows, gate_col, w_gate, w_up, w_down, filled):
    experts, rows, width = s_rows.shape
    row_spec = pl.BlockSpec((1, tile, width), lambda e, r: (e, first_tile + r, 0))
    near_spec = pl.BlockSpec((1, tile, width), lambda e, r: (e, r, 0))
    col_spec = pl.BlockSpec((1, tile, 1), lambda e, r: (e, first_tile + r, 0))
    near_col_spec = pl.BlockSpec((1, tile, 1), lambda e, r: (e, r, 0))
    w_spec = pl.BlockSpec((1, width, width), lambda e, r: (e, 0, 0))
    full = jax.ShapeDtypeStruct((experts, rows, width), jnp.bfloat16)
    out_shape, out_specs = [full] * 3, [row_spec] * 3
    args, in_specs = [s_rows, dy_rows], [row_spec, row_spec]
    aliases = {}
    if own:
        args.append(gate_col)
        in_specs.append(col_spec)
        out_shape += [full, jax.ShapeDtypeStruct((experts, num_tiles * tile, width), jnp.bfloat16),
                      jax.ShapeDtypeStruct((experts, num_tiles * tile, 1), jnp.float32)]
        out_specs += [row_spec, near_spec, near_col_spec]
        aliases[1] = 3
    args += [w_gate, w_up, w_down]
    in_specs += [w_spec] * 3
    held = () if filled is None else tuple(filled)
    for i, arr in enumerate(held):
        aliases[len(args)] = i
        args.append(arr)
        in_specs.append(pl.BlockSpec(memory_space=pl.ANY))
    units = 6 if own else 3
    return pl.pallas_call(
        functools.partial(expert_kernel, own=own, chunk=min(256, width), held=len(held)),
        out_shape=out_shape, grid=(experts, num_tiles), in_specs=in_specs, out_specs=out_specs,
        input_output_aliases=aliases,
        compiler_params=pltpu.CompilerParams(vmem_limit_bytes=VMEM_MAX, dimension_semantics=('arbitrary', 'arbitrary')),
        cost_estimate=pl.CostEstimate(flops=2 * units * experts * num_tiles * tile * width * width,
                                      bytes_accessed=2 * experts * width * (3 * width + 7 * num_tiles * tile),
                                      transcendentals=experts * num_tiles * tile * width),
        name='expert_own' if own else 'expert_far',
    )(*args)


def weight_grad_kernel(*refs, count):
    left_ref, rights, outs = refs[0], refs[1:1 + count], refs[1 + count:]
    for right_ref, out_ref in zip(rights, outs):
        out_ref[0] = dot_tn(left_ref[0], right_ref[0])


def weight_grads(left, *rights):
    experts, rows, width = left.shape
    count = len(rights)
    row_spec = pl.BlockSpec((1, rows, width), lambda e: (e, 0, 0))
    out_spec = pl.BlockSpec((1, width, width), lambda e: (e, 0, 0))
    return pl.pallas_call(
        functools.partial(weight_grad_kernel, count=count),
        out_shape=[jax.ShapeDtypeStruct((experts, width, width), jnp.float32)] * count,
        grid=(experts,), in_specs=[row_spec] * (1 + count), out_specs=[out_spec] * count,
        compiler_params=pltpu.CompilerParams(vmem_limit_bytes=VMEM_MAX, dimension_semantics=('arbitrary',)),
        cost_estimate=pl.CostEstimate(flops=2 * count * experts * rows * width * width,
                                      bytes_accessed=experts * width * (2 * (1 + count) * rows + 4 * count * width), transcendentals=0),
        name='weight_grads',
    )(left, *rights)


def combine_kernel(home_ref, begin_ref, count_ref, most_ref, ds_ref, dg_ref, slot_ref, *rest, experts, blocks, capacity, dev_from, pairs):
    out_ref, dgt_ref = rest[-2:]
    dev = pl.program_id(0) + dev_from
    row_iota = lax.broadcasted_iota(jnp.int32, (WIN, TOK_BLOCK), 0)

    def window(e, sub, first, floor=None):
        slot_row = slot_ref[0, sub, e:e + 1, :]
        hit = slot_row == row_iota + first
        if floor is not None:
            hit = hit & (slot_row >= floor)
        rows = pl.ds(pl.multiple_of(first, ALIGN), WIN)
        gate_row = jnp.sum(jnp.where(hit, dg_ref[e, 0, rows, :], 0.0), axis=0, keepdims=True)
        return jnp.where(hit, 1.0, 0.0).astype(jnp.bfloat16), ds_ref[e, 0, rows, :], gate_row

    for sub in range(pairs):
        blk = pl.program_id(1) * pairs + sub
        tokens = slice(sub * TOK_BLOCK, (sub + 1) * TOK_BLOCK)
        parts = [window(e, sub, window_start(begin_ref[(dev * experts + e) * blocks + blk], capacity)) for e in range(experts)]
        out_ref[tokens, :] = dot_tn(jnp.concatenate([p[0] for p in parts], axis=0), jnp.concatenate([p[1] for p in parts], axis=0))
        for e in range(experts):
            dgt_ref[0, sub, e:e + 1, :] = parts[e][2]

    for sub in range(pairs):
        blk = pl.program_id(1) * pairs + sub
        tokens = slice(sub * TOK_BLOCK, (sub + 1) * TOK_BLOCK)

        @pl.when(most_ref[dev * blocks + blk] > 1)
        def _():
            def per_expert(e, outer):
                at = (dev * experts + e) * blocks + blk

                def extra(w, carry):
                    floor = window_start(begin_ref[at], capacity) + w * WIN
                    first = jnp.minimum(floor, capacity - WIN)
                    rows = pl.ds(pl.multiple_of(first, ALIGN), WIN)
                    slot_row = slot_ref[0, sub, pl.ds(e, 1), :]
                    hit = (slot_row == row_iota + first) & (slot_row >= floor)
                    out_ref[tokens, :] += dot_tn(jnp.where(hit, 1.0, 0.0).astype(jnp.bfloat16), ds_ref[e, 0, rows, :])
                    dgt_ref[0, sub, pl.ds(e, 1), :] += jnp.sum(jnp.where(hit, dg_ref[e, 0, rows, :], 0.0), axis=0, keepdims=True)
                    return carry

                return lax.fori_loop(1, count_ref[at], extra, outer)

            lax.fori_loop(0, experts, per_expert, 0)


def combine_slots(home, routes, dev_from, num_dev, total_dev, d_slots, d_gate_slots, filled):
    slot_of, begin, win_count, _, most, _ = routes
    experts, _, capacity, width = d_slots.shape
    blocks = slot_of.shape[1]
    num_tokens = blocks * TOK_BLOCK
    pairs = 2 if blocks % 2 == 0 else 1

    def home_of(d, home_ref):
        return lax.bitwise_xor(d + dev_from, home_ref[0])

    held = () if filled is None else tuple(filled)
    return pl.pallas_call(
        functools.partial(combine_kernel, experts=experts, blocks=blocks, capacity=capacity, dev_from=dev_from, pairs=pairs),
        out_shape=[jax.ShapeDtypeStruct((total_dev * num_tokens, width), jnp.float32),
                   jax.ShapeDtypeStruct((total_dev, blocks, experts, TOK_BLOCK), jnp.float32)],
        grid_spec=pltpu.PrefetchScalarGridSpec(
            num_scalar_prefetch=4, grid=(num_dev, blocks // pairs),
            in_specs=[pl.BlockSpec((experts, 1, capacity, width), lambda d, b, *_: (0, d, 0, 0)),
                      pl.BlockSpec((experts, 1, capacity, 1), lambda d, b, *_: (0, d, 0, 0)),
                      pl.BlockSpec((1, pairs, experts, TOK_BLOCK), lambda d, b, *_: (d + dev_from, b, 0, 0))]
                     + [pl.BlockSpec(memory_space=pl.ANY)] * len(held),
            out_specs=[pl.BlockSpec((pairs * TOK_BLOCK, width), lambda d, b, home_ref, *_: (home_of(d, home_ref) * (blocks // pairs) + b, 0)),
                       pl.BlockSpec((1, pairs, experts, TOK_BLOCK), lambda d, b, home_ref, *_: (home_of(d, home_ref), b, 0, 0))]),
        input_output_aliases={7 + i: i for i in range(len(held))},
        compiler_params=pltpu.CompilerParams(vmem_limit_bytes=VMEM_MAX, dimension_semantics=('arbitrary', 'arbitrary')),
        cost_estimate=pl.CostEstimate(flops=2 * num_dev * blocks * experts * WIN * TOK_BLOCK * width,
                                      bytes_accessed=2 * num_dev * (2 * num_tokens + experts * capacity) * width, transcendentals=0),
        name='combine_slots',
    )(home, begin, win_count, most, d_slots, d_gate_slots, slot_of, *held)


def solution(mesh):
    ep_size, dp_size = mesh.shape['ep'], mesh.shape['dp']
    num_dev = ep_size * dp_size
    tok_spec = P(('dp', 'ep'), None, None)
    rep_spec = P()
    exp_spec = P('ep', None, None)

    def swap(value, distance):
        return lax.ppermute(value, ('dp', 'ep'), [(r, r ^ distance) for r in range(num_dev)])

    def spread_routes(value):
        return [value] + [swap(value, distance) for distance in range(1, num_dev)]

    def local_step(x_tokens, dy_tokens, route_idx, norm1_gain, norm2_gain, w_qkv, w_attn_out, w_router, w_gate, w_up, w_down):
        num_seqs, seq_len, model_width = x_tokens.shape
        num_tokens = num_seqs * seq_len
        top_k = route_idx.shape[-1]
        local_experts = w_gate.shape[0]
        num_experts = local_experts * ep_size
        capacity = capacity_rows(num_tokens, top_k, num_experts)
        x_rows = x_tokens.reshape(num_tokens, model_width)
        dy_rows = dy_tokens.reshape(num_tokens, model_width)
        idx_rows = route_idx.reshape(num_tokens, top_k)
        ep_rank = lax.axis_index('ep')
        me = lax.axis_index('dp') * ep_size + ep_rank
        first_expert = ep_rank * local_experts

        dy_all = lax.all_gather(dy_rows, ('dp', 'ep'), axis=0, tiled=True)
        idx_parts = spread_routes(idx_rows.T)
        dy_pair = swap(dy_rows, 1)
        routes = slot_positions(jnp.stack(idx_parts), first_expert, local_experts, capacity)

        cos_t, sin_t = rope_tables(seq_len)
        gain1, gain2 = norm1_gain.astype(jnp.float32)[None, :], norm2_gain.astype(jnp.float32)[None, :]
        router_pad = jnp.pad(w_router, ((0, 0), (0, -num_experts % 128)))
        normed1_t, qkv_rot = qkv_project(x_rows, gain1, w_qkv, cos_t, sin_t)
        qkv_rot, routes = lax.optimization_barrier((qkv_rot, routes))
        context = attend(qkv_rot, num_seqs)
        h_rows, normed2, probs, gate_blk = route_tokens(context, w_attn_out, x_rows, gain2, router_pad, idx_rows, ep_size, local_experts)
        x_pair = swap(normed2, 1)
        x_all = lax.all_gather(normed2, ('dp', 'ep'), axis=0, tiled=True)
        gate_for = [lax.dynamic_index_in_dim(gate_blk, jnp.bitwise_xor(ep_rank, d), axis=0, keepdims=False) for d in range(ep_size)]
        gate_parts = [gate_for[0]] + [swap(gate_for[d % ep_size], d) for d in range(1, num_dev)]
        gate_near, gate_x, gate_far = (jnp.stack(gate_parts[lo:hi]) for lo, hi in ((0, 2), (2, ep_size), (ep_size, num_dev)))

        gather = functools.partial(gather_slots, me[None], routes, own_dev=ep_size, capacity=capacity)
        rows_of = lambda a: a.reshape(local_experts, -1, a.shape[-1])
        slots_of = lambda a, n: a.reshape(local_experts, n, capacity, a.shape[-1])
        combine = functools.partial(combine_slots, ep_rank[None], routes, total_dev=ep_size)
        weights = (w_gate, w_up, w_down)
        tile = 2 * capacity
        arrays = gather(0, 1, gate_near[:1], normed2, dy_rows, None, scaled=False, from_all=False)
        s_arr, dy_arr, g_arr = gather(1, 1, gate_near[1:], x_pair, dy_pair, arrays, scaled=False, from_all=False)
        hidden, dag, dau, d_out, ds_near, dg_near = expert_pass(True, tile, 0, 1, rows_of(s_arr), rows_of(dy_arr), rows_of(g_arr), *weights, None)
        combined = combine(0, 2, d_slots=slots_of(ds_near, 2), d_gate_slots=slots_of(dg_near, 2), filled=None)
        s_arr, dy_arr, g_arr = gather(2, 2, gate_x, x_all, dy_all, (s_arr, slots_of(d_out, num_dev), g_arr), scaled=False, from_all=True)
        hidden, dag, dau, d_out, ds_x, dg_x = expert_pass(True, tile, 1, 1, rows_of(s_arr), rows_of(dy_arr), rows_of(g_arr), *weights, (hidden, dag, dau))
        d_tok, d_gate_t = combine(2, 2, d_slots=slots_of(ds_x, 2), d_gate_slots=slots_of(dg_x, 2), filled=combined)
        d_normed2_moe = lax.psum_scatter(d_tok, 'ep', scatter_dimension=0, tiled=True)
        d_gate_blk = lax.all_to_all(d_gate_t, 'ep', 0, 0, tiled=True)
        d_out, _ = lax.optimization_barrier((d_out, d_tok))
        s_arr, dy_arr = gather(4, 4, gate_far, x_all, dy_all, (s_arr, slots_of(d_out, num_dev)), scaled=True, from_all=True)
        s_all, d_out = rows_of(s_arr), rows_of(dy_arr)
        hidden, dag, dau = expert_pass(False, 2 * tile, 1, 1, s_all, d_out, None, *weights, (hidden, dag, dau))
        hidden, d_normed2_moe = lax.optimization_barrier((hidden, d_normed2_moe))
        d_w_down, = weight_grads(hidden, d_out)

        d_h, d_context, d_w_router, d_norm2_gain, d_w_attn_out = attn_out_grad(d_normed2_moe, probs, idx_rows, d_gate_blk, h_rows, normed2, context,
                                                                               dy_rows, gain2, router_pad, w_attn_out)
        d_qkv = attend_back(qkv_rot, d_context, cos_t, sin_t, num_seqs)
        d_x, d_norm1_gain = input_grad(d_qkv, w_qkv, x_rows, gain1, d_h)
        d_w_qkv = qkv_grad(normed1_t, d_qkv)
        small = jnp.concatenate([d_w_router[:, :num_experts], d_norm1_gain.T, d_norm2_gain.T], axis=1)
        dense_grads = (d_w_qkv, d_w_attn_out, small)
        d_w_qkv, d_w_attn_out, small = lax.psum(dense_grads, ('dp', 'ep'))
        s_all, dag, dau, _ = lax.optimization_barrier((s_all, dag, dau, d_qkv))
        d_w_gate, d_w_up = weight_grads(s_all, dag, dau)
        return (d_x.reshape(x_tokens.shape), small[:, num_experts], small[:, num_experts + 1], d_w_qkv, d_w_attn_out, small[:, :num_experts],
                d_w_gate, d_w_up, d_w_down)

    return jax.shard_map(local_step, mesh=mesh,
                         in_specs=(tok_spec, tok_spec, tok_spec, rep_spec, rep_spec, rep_spec, rep_spec, rep_spec, exp_spec, exp_spec, exp_spec),
                         out_specs=(tok_spec, rep_spec, rep_spec, rep_spec, rep_spec, rep_spec, exp_spec, exp_spec, exp_spec),
                         check_vma=False)
```
